32 devices in a mesh: dp: 8 (over z, y), tensor: 4 (over x, core).
Axes of the slice: x: 2, y: 2, z: 4, core: 2. Of those that a mesh axis runs over, the one named last changes fastest.
Arguments:
- tokens: bfloat16 [8192, 1024], P('dp'), may hold values from -6 to 6
- w_query: bfloat16 [1024, 1024], P(None, 'tensor'), may hold values from -0.25 to 0.25
- key_weight: bfloat16 [1024, 512], P(None, 'tensor'), may hold values from -0.25 to 0.25
- value_weight: bfloat16 [1024, 512], P(None, 'tensor'), may hold values from -0.1875 to 0.1875
- w_output: bfloat16 [1024, 1024], P('tensor'), may hold values from -1 to 1
- gain_attn: float32 [1024], replicated, may hold values from 0.5 to 1.5
- gain_ffn: float32 [1024], replicated, may hold values from 0.5 to 1.5
- router: bfloat16 [1024, 16], replicated, may hold values from -0.09375 to 0.09375
- w_gate: bfloat16 [16, 1024, 512], P(None, None, 'tensor'), may hold values from -0.1875 to 0.1875
- w_up: bfloat16 [16, 1024, 512], P(None, None, 'tensor'), may hold values from -0.1875 to 0.1875
- w_down: bfloat16 [16, 512, 1024], P(None, 'tensor'), may hold values from -1 to 1
- piece_start: int32 [8, 2], P('dp'), may hold values from 0 to 768, as said below
- piece_kind: int32 [8, 2], P('dp'), may hold values from 0 to 1
- choices: int32 [8192, 8], P('dp'), may hold values from 0 to 15, all different within a row
- place_order: int32 [8, 1024], P('dp'), may hold values from 0 to 1023, each once within a row
- cotangent: bfloat16 [8192, 1024], P('dp'), may hold values from -6 to 6
Outputs:
- output: bfloat16 [8192, 1024], P('dp')
- input_grad: bfloat16 [8192, 1024], P('dp')
- grad_query: float32 [1024, 1024], P('dp', 'tensor')
- grad_key: float32 [1024, 512], P('dp', 'tensor')
- grad_value: float32 [1024, 512], P('dp', 'tensor')
- grad_output: float32 [1024, 1024], P('tensor', 'dp')
- grad_gain_attn: float32 [1024], P('dp')
- grad_gain_ffn: float32 [1024], P('dp')
- grad_router: float32 [1024, 16], P('dp')
- grad_gate: float32 [16, 1024, 512], P(None, 'dp', 'tensor')
- grad_up: float32 [16, 1024, 512], P(None, 'dp', 'tensor')
- grad_down: float32 [16, 512, 1024], P(None, 'tensor', 'dp')
The draws below stay inside these ranges and needn't reach their ends.
Inputs may be any that keep to these rules, and one draw needn't show every extreme that they name: `piece_start`: slot k of a sequence starts in [k * 512, (k + 1) * 512 - 256], so pieces never meet. `choices`: each row names 8 different experts. `place_order`: each row is a permutation of 0 to 1023.
All inputs are finite; a program needn't handle non-finite values.
Results may differ from the reference program's by a relative error of at most 0.025.
Values may be sent and summed in bfloat16 or wider, within the bound.
A program may use at most 384 MiB of HBM per device.

```python
import jax
import jax.numpy as jnp
from jax import lax

MODEL_WIDTH = 1024
QUERY_HEADS = 16
KEY_VALUE_HEADS = 8
HEAD_SIZE = 64
FF = 512
TOP = 8
E = 16
SEQ = 1024
PIECE = 256
NPIECE = 2
QBLK = 512
SEQS = 8
TOKENS = 8192
CAP = 640


def draw_piece_start(key, part):
    region = SEQ // NPIECE
    reach_most = region - PIECE
    offsets = jax.random.randint(key, (SEQS, NPIECE), 0, reach_most + 1)
    offsets = offsets.at[0, 0].set(0).at[0, NPIECE - 1].set(reach_most)
    bases = jnp.arange(NPIECE, dtype=jnp.int32)[None, :] * region
    return (offsets + bases).astype(jnp.int32)


def place_ends(array, stream_key, low, largest):
    longest = array.shape.index(max(array.shape))
    spots = []
    for shift in (0, 1):
        where = [jax.random.randint(jax.random.fold_in(stream_key, axis), (), 0, length) for axis, length in enumerate(array.shape)]
        where[longest] = (where[longest] + shift) % array.shape[longest]
        spots.append(tuple(where))
    return array.at[spots[0]].set(low).at[spots[1]].set(largest)


def strengthened(values, stream_key, source, target, shards_of, factor):
    def block_of(dim):
        return (jnp.arange(values.shape[dim]) // (values.shape[dim] // shards_of)).reshape((-1,) + (1,) * (values.ndim - 1 - dim))

    near = jax.random.permutation(stream_key, shards_of)[block_of(target)]
    second = (block_of(target) + shards_of // 2) % shards_of
    return jnp.where((block_of(source) == near) | (block_of(source) == second), factor * values, values)


def block_scale(own_key, extent, split, least, top_value):
    def one(dim, shards_of):
        draws = jax.random.uniform(jax.random.fold_in(jax.random.fold_in(own_key, 6), dim), (shards_of,), jnp.float32, least / len(split), top_value / len(split))
        return jnp.repeat(jnp.exp(draws), extent[dim] // shards_of).reshape((-1,) + (1,) * (len(extent) - dim - 1))

    level = one(*split[0])
    for cut in split[1:]:
        level = level * one(*cut)
    return level


def picks_of(key, rows, count, top, lift):
    order = jax.random.permutation(jax.random.fold_in(key, 1), count)
    favour = order
    for power in range(3):
        favour = favour * favour // count
    favour = favour * lift // count
    chance = jax.random.randint(jax.random.fold_in(key, 2), (rows, count), 0, 4096) + favour
    fixed_rows = jax.random.permutation(jax.random.fold_in(key, 3), rows)[jnp.arange(count) % rows]
    chance = jnp.where(jnp.arange(rows)[:, None] == fixed_rows[None, :], 1 << 14, chance)
    priority = chance * count + jnp.arange(count)
    return lax.top_k(priority.astype(jnp.int32), top)[1].astype(jnp.int32)


def gaussian(own_key, dims, deviation, most, cuts=(), held_as=jnp.bfloat16):
    entries = jax.random.normal(own_key, dims, jnp.float32) * deviation
    if len(cuts) > 0:
        entries = block_scale(own_key, dims, cuts, -0.22, 0.18) * entries
    return jnp.clip(entries, min=-most, max=most).astype(held_as)


def noise_with(stream_key, dims, deviation, bound, split, heavy, held_as=jnp.bfloat16):
    array = deviation * jax.random.normal(stream_key, dims, jnp.float32)
    if split:
        array = array * block_scale(stream_key, dims, split, -0.22, 0.18)
    return jnp.clip(strengthened(array, jax.random.fold_in(stream_key, 3), *heavy), -bound, bound).astype(held_as)


def setup_inputs(seed: int = 0) -> dict:
    splits = jax.random.split(jax.random.key(seed), 17)
    tokens = gaussian(splits[0], (TOKENS, MODEL_WIDTH), 1.0, 6.0, ((0, 8),))
    w_query = gaussian(splits[1], (MODEL_WIDTH, QUERY_HEADS * HEAD_SIZE), (MODEL_WIDTH // 2) ** -0.5, 0.25, ((1, 4),))
    key_weight = gaussian(splits[2], (MODEL_WIDTH, KEY_VALUE_HEADS * HEAD_SIZE), (MODEL_WIDTH // 2) ** -0.5, 0.25, ((1, 4),))
    value_weight = gaussian(splits[3], (MODEL_WIDTH, KEY_VALUE_HEADS * HEAD_SIZE), MODEL_WIDTH ** -0.5, 0.1875, ((1, 4),))
    w_output = gaussian(splits[4], (QUERY_HEADS * HEAD_SIZE, MODEL_WIDTH), (QUERY_HEADS * HEAD_SIZE // 32) ** -0.5, 1.0, ((0, 4),))
    gain_attn = jnp.clip(1.0 + 0.1 * jax.random.normal(splits[5], (MODEL_WIDTH,), jnp.float32), 0.5, 1.5)
    gain_ffn = jnp.clip(1.0 + 0.1 * jax.random.normal(splits[6], (MODEL_WIDTH,), jnp.float32), 0.5, 1.5)
    router = gaussian(splits[7], (MODEL_WIDTH, E), (4 * MODEL_WIDTH) ** -0.5, 0.09375)
    w_gate = gaussian(splits[8], (E, MODEL_WIDTH, FF), MODEL_WIDTH ** -0.5, 0.1875, ((2, 4),))
    w_up = gaussian(splits[9], (E, MODEL_WIDTH, FF), MODEL_WIDTH ** -0.5, 0.1875, ((2, 4),))
    w_down = gaussian(splits[10], (E, FF, MODEL_WIDTH), (FF // 16) ** -0.5, 1.0, ((1, 4),))
    piece_start = draw_piece_start(jax.random.fold_in(splits[16], 71), 0)
    piece_kind = place_ends(jax.random.randint(splits[12], (SEQS, NPIECE), 0, 2), jax.random.fold_in(splits[12], 1), 0, 1).astype(jnp.int32)
    choices = picks_of(splits[13], TOKENS, E, TOP, 4096)
    place_order = jax.vmap(lambda own: jax.random.permutation(own, SEQ))(jax.random.split(splits[14], SEQS)).reshape((SEQS, SEQ)).astype(jnp.int32)
    cotangent = noise_with(splits[15], (TOKENS, MODEL_WIDTH), 1.0, 6.0, ((0, 8),), (0, 1, 8, 2.0))
    return {"tokens": tokens, "w_query": w_query, "key_weight": key_weight, "value_weight": value_weight, "w_output": w_output, "gain_attn": gain_attn, "gain_ffn": gain_ffn, "router": router, "w_gate": w_gate, "w_up": w_up, "w_down": w_down, "piece_start": piece_start, "piece_kind": piece_kind, "choices": choices, "place_order": place_order, "cotangent": cotangent}


@jax.custom_vjp
def lower_precision(v):
    return lax.optimization_barrier(v.astype(jnp.bfloat16)).astype(jnp.float32)

@jax.custom_vjp
def lower_backward(v):
    return v

def low_keep(v):
    return (lower_precision(v), None)

def low_pass(kept, grad):
    return (grad,)

def back_keep(v):
    return (v, None)

def back_low(kept, grad):
    return (lower_precision(grad),)
lower_precision.defvjp(low_keep, low_pass)
lower_backward.defvjp(back_keep, back_low)
epsilon = 1e-06
negative = -1e+30
highest = lax.Precision.HIGHEST

def product_highest(left, right):
    return jnp.dot(left, right, precision=highest, preferred_element_type=jnp.float32)

def rope_tables(sequence_length):
    half_width = HEAD_SIZE // 2
    frequency = 10000.0 ** (-(jnp.arange(half_width, dtype=jnp.float32) * 2.0 / HEAD_SIZE))
    angles = jnp.arange(sequence_length, dtype=jnp.float32)[:, None] * frequency[None, :]
    return (jnp.cos(angles), jnp.sin(angles))

def apply_rotation(values, cosine_table, sine_values):
    half_width = HEAD_SIZE // 2
    first = values[..., :half_width]
    second = values[..., half_width:]
    cos_part = cosine_table[:, None, :]
    sin_part = sine_values[:, None, :]
    return jnp.concatenate([first * cos_part - second * sin_part, second * cos_part + first * sin_part], axis=-1)

def allowed(starts, kind_row, row_pos, col_pos):
    ends = starts + PIECE
    inside_row = (kind_row[None, :] == 1) & (row_pos[:, None] >= starts[None, :]) & (row_pos[:, None] < ends[None, :])
    inside_col = (kind_row[None, :] == 1) & (col_pos[:, None] >= starts[None, :]) & (col_pos[:, None] < ends[None, :])
    same_piece = jnp.any(inside_row[:, None, :] & inside_col[None, :, :], axis=-1)
    return (col_pos[None, :] <= row_pos[:, None]) | same_piece

def slot_table(pick_rows, rank_rows):
    sequence_length = pick_rows.shape[0]
    inverse = jnp.zeros((sequence_length,), jnp.int32).at[rank_rows].set(jnp.arange(sequence_length, dtype=jnp.int32))
    ranked = pick_rows[inverse].reshape(-1)
    onehot = (ranked[:, None] == jnp.arange(E, dtype=jnp.int32)[None, :]).astype(jnp.int32)
    before = jnp.cumsum(onehot, axis=0) - onehot
    return lax.optimization_barrier(jnp.sum(before * onehot, axis=1)).reshape(sequence_length, TOP)[rank_rows]

def routing(pick_rows, rank_rows):
    sequence_length = pick_rows.shape[0]
    slot_index = slot_table(pick_rows, rank_rows)
    kept = slot_index < CAP
    flat_index = jnp.where(kept, pick_rows * CAP + slot_index, E * CAP).astype(jnp.int32)
    owners = jnp.broadcast_to(jnp.arange(sequence_length, dtype=jnp.int32)[:, None], pick_rows.shape)
    token_table = jnp.full((E * CAP + 1,), sequence_length, jnp.int32).at[flat_index.reshape(-1)].set(owners.reshape(-1))
    return (flat_index, kept, token_table[:E * CAP])

def layer(resid_in, params, starts, kind_row, pick_rows, rank_rows):
    w_query, key_weight, value_weight, w_output, gain_attn, gain_ffn, router, w_gate, w_up, w_down = params
    sequence_length = resid_in.shape[0]
    head_groups = QUERY_HEADS // KEY_VALUE_HEADS
    inv_one = lax.rsqrt(lax.optimization_barrier(jnp.mean(resid_in * resid_in, axis=1, keepdims=True)) + epsilon)
    first_normed = lower_precision(resid_in * inv_one * gain_attn)
    cosine_table, sine_values = rope_tables(sequence_length)
    query_unrotated = lower_backward(product_highest(first_normed, w_query)).reshape(sequence_length, QUERY_HEADS, HEAD_SIZE)
    query_rows = lower_precision(apply_rotation(query_unrotated, cosine_table, sine_values)).reshape(sequence_length, KEY_VALUE_HEADS, head_groups, HEAD_SIZE)
    key_unrotated = lower_backward(product_highest(first_normed, key_weight)).reshape(sequence_length, KEY_VALUE_HEADS, HEAD_SIZE)
    key_rows = lower_precision(apply_rotation(key_unrotated, cosine_table, sine_values))
    value_matrix_rows = lower_precision(lower_backward(product_highest(first_normed, value_weight))).reshape(sequence_length, KEY_VALUE_HEADS, HEAD_SIZE)
    col_pos = jnp.arange(sequence_length, dtype=jnp.int32)

    def attend(block_index):
        start_row = block_index * QBLK
        query_block = lax.dynamic_slice_in_dim(query_rows, start_row, QBLK, 0)
        scores = jnp.einsum('qgrd,kgd->grqk', query_block, key_rows, precision=highest) * HEAD_SIZE ** (-0.5)
        scores = lower_backward(scores)
        visible = allowed(starts, kind_row, start_row + jnp.arange(QBLK, dtype=jnp.int32), col_pos)
        scores = jnp.where(visible[None, None], scores, negative)
        attn_probs = lower_precision(jax.nn.softmax(scores, axis=-1))
        return jnp.einsum('grqk,kgd->qgrd', attn_probs, value_matrix_rows, precision=highest)
    head_out = lax.map(jax.checkpoint(attend), jnp.arange(sequence_length // QBLK, dtype=jnp.int32))
    head_out = lower_precision(lower_backward(head_out.reshape(sequence_length, QUERY_HEADS * HEAD_SIZE)))
    resid_mid = resid_in + lower_backward(product_highest(head_out, w_output))
    inv_two = lax.rsqrt(lax.optimization_barrier(jnp.mean(resid_mid * resid_mid, axis=1, keepdims=True)) + epsilon)
    normed_two = lower_precision(resid_mid * inv_two * gain_ffn)
    logits = lower_backward(product_highest(normed_two, router))
    gate_probs = jax.nn.softmax(jnp.take_along_axis(logits, pick_rows, axis=1), axis=1)
    flat_index, kept, token_table = routing(pick_rows, rank_rows)
    padded_in = jnp.concatenate([normed_two, jnp.zeros((1, MODEL_WIDTH), normed_two.dtype)], axis=0)
    dispatched = padded_in[token_table].reshape(E, CAP, MODEL_WIDTH)
    gate_pre = lower_backward(jnp.einsum('ecd,edf->ecf', dispatched, w_gate, precision=highest))
    up_pre = lower_backward(jnp.einsum('ecd,edf->ecf', dispatched, w_up, precision=highest))
    hidden = lower_precision(jax.nn.silu(gate_pre) * up_pre)
    expert_out = lower_backward(jnp.einsum('ecf,efd->ecd', hidden, w_down, precision=highest)).reshape(E * CAP, MODEL_WIDTH)
    padded_out = jnp.concatenate([expert_out, jnp.zeros((1, MODEL_WIDTH), expert_out.dtype)], axis=0)
    gathered = padded_out[flat_index]
    slot_gate = gate_probs * kept.astype(gate_probs.dtype)
    return resid_mid + lax.optimization_barrier(jnp.sum(gathered * slot_gate[:, :, None], axis=1))

def reference(tokens, w_query, key_weight, value_weight, w_output, gain_attn, gain_ffn, router, w_gate, w_up, w_down, piece_start, piece_kind, choices, place_order, cotangent):
    weight_list = tuple((weight.astype(jnp.float32) for weight in (w_query, key_weight, value_weight, w_output, gain_attn, gain_ffn, router, w_gate, w_up, w_down)))
    resid_all = tokens.astype(jnp.float32).reshape(SEQS, SEQ, MODEL_WIDTH)
    grad_all = cotangent.astype(jnp.float32).reshape(SEQS, SEQ, MODEL_WIDTH)
    picks_all = choices.reshape(SEQS, SEQ, TOP)

    def one_sequence(totals, inputs):
        resid_seq, grad_seq, starts, kind_row, pick_rows, rank_rows = inputs

        def forward(resid_arg, *params):
            return layer(resid_arg, params, starts, kind_row, pick_rows, rank_rows)
        result, pullback = jax.vjp(forward, resid_seq, *weight_list)
        cotangents = pullback(grad_seq)
        totals = tuple((a + b for a, b in zip(totals, cotangents[1:])))
        return (totals, (result.astype(jnp.bfloat16), cotangents[0].astype(jnp.bfloat16)))
    initial = tuple((jnp.zeros_like(weight) for weight in weight_list))
    totals, (outputs, input_grads) = lax.scan(one_sequence, initial, (resid_all, grad_all, piece_start, piece_kind, picks_all, place_order))
    return (outputs.reshape(TOKENS, MODEL_WIDTH), input_grads.reshape(TOKENS, MODEL_WIDTH), totals[0], totals[1], totals[2], totals[3], totals[4], totals[5], totals[6], totals[7], totals[8], totals[9])
```

```python
import jax
import jax.numpy as jnp
from jax import lax
from jax.sharding import PartitionSpec as P

MODEL_WIDTH = 1024
HEAD_SIZE = 64
E = 16
PIECE = 256
QBLK = 512
CAP = 640

epsilon = 1e-06
negative = -1e30
F32 = jnp.float32
BF16 = jnp.bfloat16


def mm(left, right, dims):
    return lax.dot_general(left, right, (dims, ((), ())), preferred_element_type=F32)


def rope_tables(sequence_length):
    half_width = HEAD_SIZE // 2
    frequency = 10000.0 ** (-(jnp.arange(half_width, dtype=F32) * 2.0 / HEAD_SIZE))
    angles = jnp.arange(sequence_length, dtype=F32)[:, None] * frequency[None, :]
    return (jnp.cos(angles), jnp.sin(angles))


def apply_rotation(values, cosine_table, sine_values):
    half_width = HEAD_SIZE // 2
    first = values[..., :half_width]
    second = values[..., half_width:]
    cos_part = cosine_table[:, None, :]
    sin_part = sine_values[:, None, :]
    return jnp.concatenate(
        [first * cos_part - second * sin_part, second * cos_part + first * sin_part], axis=-1
    )


def unrotate(grads, cosine_table, sine_values):
    return apply_rotation(grads, cosine_table, -sine_values)


def allowed(starts, kind_row, row_pos, col_pos):
    ends = starts + PIECE
    inside_row = (
        (kind_row[None, :] == 1)
        & (row_pos[:, None] >= starts[None, :])
        & (row_pos[:, None] < ends[None, :])
    )
    inside_col = (
        (kind_row[None, :] == 1)
        & (col_pos[:, None] >= starts[None, :])
        & (col_pos[:, None] < ends[None, :])
    )
    same_piece = jnp.any(inside_row[:, None, :] & inside_col[None, :, :], axis=-1)
    return (col_pos[None, :] <= row_pos[:, None]) | same_piece


CORE_PAIRS = [(i, i ^ 1) for i in range(4)]
X_PAIRS = [(i, i ^ 2) for i in range(4)]


def reduce_half(part, core):
    half = part.shape[0] // 2
    mine = lax.dynamic_slice_in_dim(part, core * half, half, 0)
    other = lax.dynamic_slice_in_dim(part, (1 - core) * half, half, 0)
    got = lax.ppermute(other, "tensor", CORE_PAIRS)
    total = (mine.astype(F32) + got.astype(F32)).astype(part.dtype)
    far = lax.ppermute(total, "tensor", X_PAIRS)
    return total.astype(F32) + far.astype(F32)


def share_half(half_rows, core):
    got = lax.ppermute(half_rows, "tensor", CORE_PAIRS)
    pair = jnp.stack([jnp.where(core == 0, half_rows, got), jnp.where(core == 0, got, half_rows)])
    return pair.reshape((2 * half_rows.shape[0],) + half_rows.shape[1:])


def scatter_sum(blocks, ways):
    me = lax.axis_index("dp")
    if ways != 8:
        return lax.psum_scatter(blocks, "dp", scatter_dimension=0, tiled=False).astype(F32)
    y = me % 2
    z = me // 2
    grid = blocks.reshape((4, 2) + blocks.shape[1:])
    mine = lax.dynamic_index_in_dim(grid, y, 1, keepdims=False)
    other = lax.dynamic_index_in_dim(grid, 1 - y, 1, keepdims=False)
    got = lax.ppermute(other, "dp", [(i, i ^ 1) for i in range(8)])
    summed = (mine.astype(F32) + got.astype(F32)).astype(blocks.dtype)
    total = lax.dynamic_index_in_dim(summed, z, 0, keepdims=False).astype(F32)
    for step in (1, 2, 3):
        block = lax.dynamic_index_in_dim(summed, (z + step) % 4, 0, keepdims=False)
        arrived = lax.ppermute(
            block, "dp", [(i, (i + 2 * step) % 8) for i in range(8)]
        )
        total = total + arrived.astype(F32)
    return total


def make_body(ways):
    def body(
        tokens,
        w_query,
        key_weight,
        value_weight,
        w_output,
        gain_attn,
        gain_ffn,
        router,
        w_gate,
        w_up,
        w_down,
        piece_start,
        piece_kind,
        choices,
        place_order,
        cotangent,
    ):
        rows = tokens.shape[0]
        half = rows // 2
        width = tokens.shape[1]
        kv_local = key_weight.shape[1] // HEAD_SIZE
        q_local = w_query.shape[1] // HEAD_SIZE
        ff = w_gate.shape[2]
        group = q_local // kv_local
        scale = HEAD_SIZE ** (-0.5)
        core = lax.axis_index("tensor") % 2

        def my_half(array):
            return lax.dynamic_slice_in_dim(array, core * half, half, 0)

        resid_in = tokens.astype(F32)
        inv_one = lax.rsqrt(jnp.mean(resid_in * resid_in, axis=1, keepdims=True) + epsilon)
        first_normed = (resid_in * inv_one * gain_attn).astype(BF16)
        cos_rows, sin_rows = rope_tables(rows)
        qp = mm(first_normed, w_query, ((1,), (0,))).reshape(rows, q_local, HEAD_SIZE)
        q = apply_rotation(qp, cos_rows, sin_rows).astype(BF16)
        q = q.reshape(rows, kv_local, group, HEAD_SIZE)
        kp = mm(first_normed, key_weight, ((1,), (0,))).reshape(rows, kv_local, HEAD_SIZE)
        k = apply_rotation(kp, cos_rows, sin_rows).astype(BF16)
        v = mm(first_normed, value_weight, ((1,), (0,))).astype(BF16)
        v = v.reshape(rows, kv_local, HEAD_SIZE)
        blocks = rows // QBLK

        def block_scores(block):
            start = block * QBLK
            length = start + QBLK
            scores = (
                jnp.einsum(
                    "qgrd,kgd->grqk", q[start:length], k[:length], preferred_element_type=F32
                )
                * scale
            )
            visible = allowed(
                piece_start[0],
                piece_kind[0],
                start + jnp.arange(QBLK, dtype=jnp.int32),
                jnp.arange(length, dtype=jnp.int32),
            )
            return jnp.where(visible[None, None], scores, negative)

        outs, totals = [], []
        for block in range(blocks):
            scores = block_scores(block)
            top = jnp.max(scores, axis=-1, keepdims=True)
            total = top + jnp.log(jnp.sum(jnp.exp(scores - top), axis=-1, keepdims=True))
            probs = jnp.exp(scores - total).astype(BF16)
            length = (block + 1) * QBLK
            res = jnp.einsum("grqk,kgd->qgrd", probs, v[:length], preferred_element_type=F32)
            outs.append(res.astype(BF16))
            totals.append(total)
        head_out = jnp.concatenate(outs, axis=0).reshape(rows, q_local * HEAD_SIZE)
        attn_part = mm(head_out, w_output, ((1,), (0,))).astype(BF16)
        mid = my_half(resid_in) + reduce_half(attn_part, core)
        inv_two = lax.rsqrt(jnp.mean(mid * mid, axis=1, keepdims=True) + epsilon)
        normed_half = (mid * inv_two * gain_ffn).astype(BF16)
        normed = share_half(normed_half, core)

        expert_ids = jnp.arange(E, dtype=jnp.int32)
        picked = jnp.any(choices[:, :, None] == expert_ids[None, None, :], axis=1)
        ranks = place_order[0]
        earlier = (ranks[None, :] < ranks[:, None]).astype(BF16)
        slot = mm(earlier, picked.astype(BF16), ((1,), (0,)))
        kept = (picked & (slot < CAP)).astype(F32)
        logits = mm(normed, router, ((1,), (0,)))
        logits = jnp.where(picked, logits, negative)
        gates = jax.nn.softmax(logits, axis=1)
        gates = jnp.where(picked, gates, 0.0)
        slot_gate = gates * kept

        gate_pre = jnp.einsum("td,edf->tef", normed, w_gate, preferred_element_type=F32)
        up_pre = jnp.einsum("td,edf->tef", normed, w_up, preferred_element_type=F32)
        dy_down = jnp.einsum("td,efd->tef", cotangent, w_down, preferred_element_type=F32)
        sigmoid = jax.nn.sigmoid(gate_pre)
        act = gate_pre * sigmoid
        hidden = act * up_pre
        gated = (slot_gate[:, :, None] * hidden).astype(BF16)
        grad_gate_part = jnp.sum(hidden * dy_down, axis=2) * kept
        grad_hidden = slot_gate[:, :, None] * dy_down
        slope = sigmoid * (1.0 + gate_pre * (1.0 - sigmoid))
        grad_a = (grad_hidden * up_pre * slope).astype(BF16)
        grad_u = (grad_hidden * act).astype(BF16)
        moe_part = jnp.einsum("tef,efd->td", gated, w_down, preferred_element_type=F32)
        norm_part = jnp.einsum("tef,edf->td", grad_a, w_gate, preferred_element_type=F32)
        norm_part = norm_part + jnp.einsum("tef,edf->td", grad_u, w_up, preferred_element_type=F32)
        piece = width // ways
        grad_gate = jnp.einsum("td,tef->edf", normed, grad_a, preferred_element_type=F32)
        grad_up = jnp.einsum("td,tef->edf", normed, grad_u, preferred_element_type=F32)
        grad_down = jnp.einsum("tef,td->efd", gated, cotangent, preferred_element_type=F32)

        def send_rows(grad):
            e, d, f = grad.shape
            return grad.astype(BF16).reshape(e, ways, d // ways, f).transpose(1, 0, 2, 3)

        def send_columns(grad):
            e, f, d = grad.shape
            return grad.astype(BF16).reshape(e, f, ways, d // ways).transpose(2, 0, 1, 3)

        sent_gate = scatter_sum(send_rows(grad_gate), ways)
        sent_up = scatter_sum(send_rows(grad_up), ways)
        sent_down = scatter_sum(send_columns(grad_down), ways)

        norm_half = reduce_half(norm_part.astype(BF16), core)
        dg_half = reduce_half(grad_gate_part, core)
        output = share_half(
            (mid + reduce_half(moe_part.astype(BF16), core)).astype(BF16), core
        )
        gates_half = my_half(gates)
        dz = gates_half * (dg_half - jnp.sum(gates_half * dg_half, axis=1, keepdims=True))
        dlg = dz.astype(BF16)
        grad_norm = norm_half + mm(dlg, router, ((1,), (1,)))
        grad_router = mm(dlg, normed_half, ((0,), (0,)))
        grad_gain_ffn = jnp.sum(grad_norm * mid * inv_two, axis=0)
        scaled = gain_ffn * grad_norm
        grad_mid = (
            my_half(cotangent).astype(F32)
            + inv_two * scaled
            - mid * inv_two**3 * jnp.mean(scaled * mid, axis=1, keepdims=True)
        )
        grad_attn = share_half(grad_mid.astype(BF16), core)
        grad_output = mm(head_out, grad_attn, ((0,), (0,)))
        sent_output = scatter_sum(
            grad_output.astype(BF16).reshape(q_local * HEAD_SIZE, ways, piece).transpose(1, 0, 2),
            ways,
        )
        grad_heads = mm(grad_attn, w_output, ((1,), (1,))).astype(BF16)
        grad_heads = grad_heads.reshape(rows, kv_local, group, HEAD_SIZE)
        query_parts = []
        grad_k = jnp.zeros((rows, kv_local, HEAD_SIZE), F32)
        grad_v = jnp.zeros((rows, kv_local, HEAD_SIZE), F32)
        for block in range(blocks):
            scores = block_scores(block)
            start = block * QBLK
            length = start + QBLK
            probs = jnp.exp(scores - totals[block])
            dob = grad_heads[start:length]
            dp = jnp.einsum("qgrd,kgd->grqk", dob, v[:length], preferred_element_type=F32)
            delta = jnp.sum(probs * dp, axis=-1, keepdims=True)
            ds = (probs * (dp - delta)).astype(BF16)
            query_parts.append(
                jnp.einsum("grqk,kgd->qgrd", ds, k[:length], preferred_element_type=F32) * scale
            )
            dk = jnp.einsum("grqk,qgrd->kgd", ds, q[start:length], preferred_element_type=F32)
            dv = jnp.einsum("grqk,qgrd->kgd", probs.astype(BF16), dob, preferred_element_type=F32)
            pad = ((0, rows - length), (0, 0), (0, 0))
            grad_k = grad_k + jnp.pad(dk * scale, pad)
            grad_v = grad_v + jnp.pad(dv, pad)
        grad_q = jnp.concatenate(query_parts, axis=0).reshape(rows, q_local, HEAD_SIZE)
        dqp = unrotate(grad_q, cos_rows, sin_rows).astype(BF16).reshape(rows, -1)
        dkp = unrotate(grad_k, cos_rows, sin_rows).astype(BF16).reshape(rows, -1)
        dvb = grad_v.astype(BF16).reshape(rows, -1)
        grad_qkv = jnp.concatenate([dqp, dkp, dvb], axis=1)
        w_qkv = jnp.concatenate([w_query, key_weight, value_weight], axis=1)
        grad_wide = mm(first_normed, grad_qkv, ((0,), (0,))).astype(BF16)
        sent_qkv = scatter_sum(grad_wide.reshape(ways, piece, -1), ways)
        nq, nk = w_query.shape[1], key_weight.shape[1]
        normed_one_part = mm(grad_qkv, w_qkv, ((1,), (1,)))
        norm_one_half = reduce_half(normed_one_part.astype(BF16), core)
        x_half = my_half(resid_in)
        inv_half = my_half(inv_one)
        grad_gain_attn = jnp.sum(norm_one_half * x_half * inv_half, axis=0)
        scaled_one = gain_attn * norm_one_half
        input_half = (
            grad_mid
            + inv_half * scaled_one
            - x_half * inv_half**3 * jnp.mean(scaled_one * x_half, axis=1, keepdims=True)
        ).astype(BF16)
        input_grad = share_half(input_half, core)
        small = jnp.concatenate([grad_gain_attn[None], grad_gain_ffn[None], grad_router], axis=0)
        small = small + lax.ppermute(small, "tensor", CORE_PAIRS)
        count = small.shape[0]
        small = scatter_sum(small.reshape(count, ways, piece).transpose(1, 0, 2), ways)
        return (
            output,
            input_grad,
            sent_qkv[:, :nq],
            sent_qkv[:, nq : nq + nk],
            sent_qkv[:, nq + nk :],
            sent_output,
            small[0],
            small[1],
            small[2:].T,
            sent_gate,
            sent_up,
            sent_down,
        )

    return body


def solution(mesh):
    return jax.shard_map(
        make_body(mesh.shape["dp"]),
        mesh=mesh,
        in_specs=(
            P("dp", None),
            P(None, "tensor"),
            P(None, "tensor"),
            P(None, "tensor"),
            P("tensor", None),
            P(),
            P(),
            P(),
            P(None, None, "tensor"),
            P(None, None, "tensor"),
            P(None, "tensor", None),
            P("dp", None),
            P("dp", None),
            P("dp", None),
            P("dp", None),
            P("dp", None),
        ),
        out_specs=(
            P("dp", None),
            P("dp", None),
            P("dp", "tensor"),
            P("dp", "tensor"),
            P("dp", "tensor"),
            P("tensor", "dp"),
            P("dp"),
            P("dp"),
            P("dp", None),
            P(None, "dp", "tensor"),
            P(None, "dp", "tensor"),
            P(None, "tensor", "dp"),
        ),
        check_vma=False,
    )
```

```python
import functools

import jax
import jax.numpy as jnp
from jax import lax
from jax.experimental import pallas as pl
from jax.experimental.pallas import tpu as pltpu
from jax.sharding import PartitionSpec as P

MODEL_WIDTH = 1024
HEAD_SIZE = 64
E = 16
PIECE = 256
QBLK = 512
CAP = 640

epsilon = 1e-06
negative = -1e30
F32 = jnp.float32
BF16 = jnp.bfloat16


def mm(left, right, dims):
    return lax.dot_general(left, right, (dims, ((), ())), preferred_element_type=F32)


def rope_tables(sequence_length):
    half_width = HEAD_SIZE // 2
    frequency = 10000.0 ** (-(jnp.arange(half_width, dtype=F32) * 2.0 / HEAD_SIZE))
    angles = jnp.arange(sequence_length, dtype=F32)[:, None] * frequency[None, :]
    return (jnp.cos(angles), jnp.sin(angles))


def apply_rotation(values, cosine_table, sine_values):
    half_width = HEAD_SIZE // 2
    first = values[..., :half_width]
    second = values[..., half_width:]
    cos_part = cosine_table[:, None, :]
    sin_part = sine_values[:, None, :]
    return jnp.concatenate(
        [first * cos_part - second * sin_part, second * cos_part + first * sin_part], axis=-1
    )


def unrotate(grads, cosine_table, sine_values):
    return apply_rotation(grads, cosine_table, -sine_values)


def allowed(starts, kind_row, row_pos, col_pos):
    ends = starts + PIECE
    inside_row = (
        (kind_row[None, :] == 1)
        & (row_pos[:, None] >= starts[None, :])
        & (row_pos[:, None] < ends[None, :])
    )
    inside_col = (
        (kind_row[None, :] == 1)
        & (col_pos[:, None] >= starts[None, :])
        & (col_pos[:, None] < ends[None, :])
    )
    same_piece = jnp.any(inside_row[:, None, :] & inside_col[None, :, :], axis=-1)
    return (col_pos[None, :] <= row_pos[:, None]) | same_piece


CORE_PAIRS = [(i, i ^ 1) for i in range(4)]
X_PAIRS = [(i, i ^ 2) for i in range(4)]


def reduce_half(part, core):
    half = part.shape[0] // 2
    mine = lax.dynamic_slice_in_dim(part, core * half, half, 0)
    other = lax.dynamic_slice_in_dim(part, (1 - core) * half, half, 0).astype(BF16)
    got = lax.ppermute(other, "tensor", CORE_PAIRS)
    total = (mine + got.astype(F32)).astype(BF16)
    far = lax.ppermute(total, "tensor", X_PAIRS)
    return total.astype(F32) + far.astype(F32)


def share_half(half_rows, core):
    got = lax.ppermute(half_rows, "tensor", CORE_PAIRS)
    pair = jnp.stack([jnp.where(core == 0, half_rows, got), jnp.where(core == 0, got, half_rows)])
    return pair.reshape((2 * half_rows.shape[0],) + half_rows.shape[1:])


def bits_of(ways):
    return tuple(range(ways.bit_length() - 1))


def flip(array, ways, bit):
    return lax.ppermute(array, "dp", [(i, i ^ (1 << bit)) for i in range(ways)])


def halve(keep, send, ways, order):
    got = flip(send, ways, order[0])
    for bit in order[1:]:
        half = keep.shape[0] // 2
        to_send = (keep[half:].astype(F32) + got[half:].astype(F32)).astype(keep.dtype)
        keep = (keep[:half].astype(F32) + got[:half].astype(F32)).astype(keep.dtype)
        got = flip(to_send, ways, bit)
    return (keep.astype(F32) + got.astype(F32))[0]


def scatter_sum(blocks, ways, order):
    me = lax.axis_index("dp")
    count = len(order)
    current = blocks.reshape((2,) * count + blocks.shape[1:])
    left = list(reversed(range(count)))
    for bit in order:
        axis = left.index(bit)
        mine_at = (me >> bit) & 1
        mine = lax.dynamic_index_in_dim(current, mine_at, axis, keepdims=False)
        other = lax.dynamic_index_in_dim(current, 1 - mine_at, axis, keepdims=False)
        got = flip(other, ways, bit)
        total = mine.astype(F32) + got.astype(F32)
        left.remove(bit)
        current = total.astype(blocks.dtype) if left else total
    return current


QUAD = 4
ROWS = 256


def expert_kernel(first, quads, ways, orders, carried, *refs):
    x_ref, xt_ref, dy_ref, dyt_ref, gate_ref, wg_ref, wu_ref, wd_ref = refs[:8]
    refs = refs[8:]
    if carried:
        norm_in, moe_in = refs[:2]
        refs = refs[2:]
    dg_ref, norm_out, moe_out = refs[:3]
    keeps = refs[3 : 3 + quads]
    sends = refs[3 + quads : 3 + 2 * quads]
    wgu, gu, gated, grads, norm_acc, moe_acc, block_sem, acc_sem = refs[3 + 2 * quads :]
    step = pl.program_id(0)
    rows, width = x_ref.shape
    ff = wg_ref.shape[2]
    piece = width // ways
    me = lax.axis_index("dp")
    load_norm = load_moe = None
    if carried:
        load_norm = pltpu.make_async_copy(norm_in, norm_acc, acc_sem.at[0])
        load_moe = pltpu.make_async_copy(moe_in, moe_acc, acc_sem.at[1])

        @pl.when(step == 0)
        def _():
            load_norm.start()
            load_moe.start()

    @pl.when(step == 0)
    def _():
        dg_ref[...] = jnp.zeros_like(dg_ref)

    for j in range(QUAD):
        wgu[:, 2 * j * ff : (2 * j + 1) * ff] = wg_ref[j]
        wgu[:, (2 * j + 1) * ff : (2 * j + 2) * ff] = wu_ref[j]
    lane = lax.broadcasted_iota(jnp.int32, (ROWS, dg_ref.shape[1]), 1)

    def hidden_rows(i, _):
        at = pl.ds(pl.multiple_of(i * ROWS, ROWS), ROWS)
        au = mm(x_ref[at, :], wgu[...], ((1,), (0,)))
        down = mm(dy_ref[at, :], wd_ref[...].reshape(QUAD * ff, width), ((1,), (1,)))
        gate_rows = gate_ref[0, at, :]
        dg = dg_ref[at, :]
        for j in range(QUAD):
            pre = au[:, 2 * j * ff : (2 * j + 1) * ff]
            up = au[:, (2 * j + 1) * ff : (2 * j + 2) * ff]
            back = down[:, j * ff : (j + 1) * ff]
            gate = gate_rows[:, j : j + 1]
            sigmoid = 1.0 / (1.0 + jnp.exp(-pre))
            act = pre * sigmoid
            hidden = act * up
            gated[at, j * ff : (j + 1) * ff] = (gate * hidden).astype(BF16)
            row = jnp.sum(hidden * back, axis=1, keepdims=True)
            dg = jnp.where(lane == (first + step) * QUAD + j, row, dg)
            back = gate * back
            slope = sigmoid * (1.0 + pre * (1.0 - sigmoid))
            gu[at, 2 * j * ff : (2 * j + 1) * ff] = (back * up * slope).astype(BF16)
            gu[at, (2 * j + 1) * ff : (2 * j + 2) * ff] = (back * act).astype(BF16)
        dg_ref[at, :] = dg
        return 0

    lax.fori_loop(0, rows // ROWS, hidden_rows, 0)

    def copies(chunk):
        out = []
        for slot in range(ways):
            dest = 0
            for place, bit in enumerate(orders[chunk]):
                own = (slot >> (len(orders[chunk]) - 1 - place)) & 1
                dest = dest + ((me // (1 << bit) + own) % 2) * (1 << bit)
            block = grads.at[pl.ds(pl.multiple_of(dest * piece, piece), piece), :]
            half = ways // 2
            target = keeps[chunk].at[slot] if slot < half else sends[chunk].at[slot - half]
            out.append(pltpu.make_async_copy(block, target, block_sem.at[slot]))
        return out

    if quads > 1:

        @pl.when(step > 0)
        def _():
            for copy in copies(0):
                copy.wait()

    def grad_rows(i, _):
        at = pl.ds(pl.multiple_of(i * ROWS, ROWS), ROWS)
        grads[at, : 2 * QUAD * ff] = mm(xt_ref[at, :], gu[...], ((1,), (0,))).astype(BF16)
        grads[at, 2 * QUAD * ff :] = mm(dyt_ref[at, :], gated[...], ((1,), (0,))).astype(BF16)
        return 0

    lax.fori_loop(0, width // ROWS, grad_rows, 0)
    for chunk in range(quads):

        @pl.when(step == chunk)
        def _():
            for copy in copies(chunk):
                copy.start()

    if carried:

        @pl.when(step == 0)
        def _():
            load_norm.wait()
            load_moe.wait()

    def data_rows(i, _):
        at = pl.ds(pl.multiple_of(i * ROWS, ROWS), ROWS)
        norm = mm(gu[at, :], wgu[...], ((1,), (1,)))
        moe = mm(gated[at, :], wd_ref[...].reshape(QUAD * ff, width), ((1,), (0,)))
        if carried:
            norm_acc[at, :] += norm
            moe_acc[at, :] += moe
        else:
            norm_acc[at, :] = norm
            moe_acc[at, :] = moe
        return 0

    lax.fori_loop(0, rows // ROWS, data_rows, 0)

    @pl.when(step == quads - 1)
    def _():
        save_norm = pltpu.make_async_copy(norm_acc, norm_out, acc_sem.at[0])
        save_moe = pltpu.make_async_copy(moe_acc, moe_out, acc_sem.at[1])
        save_norm.start()
        save_moe.start()
        for copy in copies(0):
            copy.wait()
        save_norm.wait()
        save_moe.wait()


def run_experts(first, orders, ways, x, xt, dy, dyt, gates, w_gate, w_up, w_down, carry):
    quads = len(orders)
    assert carry is not None or quads == 1
    rows, width = x.shape
    ff = w_gate.shape[2]
    piece = width // ways
    whole = pl.BlockSpec((rows, width), lambda s: (0, 0), pipeline_mode=pl.Buffered(1))
    flat = pl.BlockSpec((width, rows), lambda s: (0, 0), pipeline_mode=pl.Buffered(1))
    any_space = pl.BlockSpec(memory_space=pl.ANY)
    wide = 3 * QUAD * ff
    block = jax.ShapeDtypeStruct((ways // 2, piece, wide), BF16)
    total = jax.ShapeDtypeStruct((rows, width), F32)
    flops = 2 * 9 * quads * QUAD * rows * width * ff
    moved = quads * QUAD * width * ff * 12 + rows * width * 8 + rows * width * 16
    out = pl.pallas_call(
        functools.partial(expert_kernel, first, quads, ways, orders, carry is not None),
        grid=(quads,),
        out_shape=(jax.ShapeDtypeStruct((rows, 128), F32), total, total) + (block,) * (2 * quads),
        in_specs=[
            whole,
            flat,
            whole,
            flat,
            pl.BlockSpec((1, rows, QUAD), lambda s: (first + s, 0, 0)),
            pl.BlockSpec((QUAD, width, ff), lambda s: (first + s, 0, 0)),
            pl.BlockSpec((QUAD, width, ff), lambda s: (first + s, 0, 0)),
            pl.BlockSpec((QUAD, ff, width), lambda s: (first + s, 0, 0)),
        ]
        + ([any_space] * 2 if carry is not None else []),
        out_specs=(pl.BlockSpec((rows, 128), lambda s: (0, 0)), any_space, any_space)
        + (any_space,) * (2 * quads),
        scratch_shapes=[
            pltpu.VMEM((width, 2 * QUAD * ff), BF16),
            pltpu.VMEM((rows, 2 * QUAD * ff), BF16),
            pltpu.VMEM((rows, QUAD * ff), BF16),
            pltpu.VMEM((width, wide), BF16),
            pltpu.VMEM((rows, width), F32),
            pltpu.VMEM((rows, width), F32),
            pltpu.SemaphoreType.DMA((ways,)),
            pltpu.SemaphoreType.DMA((2,)),
        ],
        compiler_params=pltpu.CompilerParams(
            dimension_semantics=("arbitrary",), vmem_limit_bytes=44 << 20
        ),
        cost_estimate=pl.CostEstimate(
            flops=flops, bytes_accessed=moved, transcendentals=quads * QUAD * rows * ff
        ),
        name="experts_" + str(first),
    )(x, xt, dy, dyt, gates, w_gate, w_up, w_down, *(carry if carry is not None else ()))
    return out[0], out[1], out[2], out[3 : 3 + quads], out[3 + quads :]


def make_body(ways):
    def body(
        tokens,
        w_query,
        key_weight,
        value_weight,
        w_output,
        gain_attn,
        gain_ffn,
        router,
        w_gate,
        w_up,
        w_down,
        piece_start,
        piece_kind,
        choices,
        place_order,
        cotangent,
    ):
        rows = tokens.shape[0]
        half = rows // 2
        width = tokens.shape[1]
        kv_local = key_weight.shape[1] // HEAD_SIZE
        q_local = w_query.shape[1] // HEAD_SIZE
        ff = w_gate.shape[2]
        group = q_local // kv_local
        scale = HEAD_SIZE ** (-0.5)
        core = lax.axis_index("tensor") % 2

        def my_half(array):
            return lax.dynamic_slice_in_dim(array, core * half, half, 0)

        from_x = lax.ppermute(w_output, "tensor", X_PAIRS)
        near = jnp.stack([w_output, from_x])
        far = lax.ppermute(near, "tensor", CORE_PAIRS)
        all_output = jnp.concatenate([w_output, far[0], from_x, far[1]], axis=0)
        resid_in = tokens.astype(F32)
        inv_one = lax.rsqrt(jnp.mean(resid_in * resid_in, axis=1, keepdims=True) + epsilon)
        first_normed = (resid_in * inv_one * gain_attn).astype(BF16)
        cos_rows, sin_rows = rope_tables(rows)
        qp = mm(first_normed, w_query, ((1,), (0,))).reshape(rows, q_local, HEAD_SIZE)
        q = apply_rotation(qp, cos_rows, sin_rows).astype(BF16)
        q = q.reshape(rows, kv_local, group, HEAD_SIZE)
        kp = mm(first_normed, key_weight, ((1,), (0,))).reshape(rows, kv_local, HEAD_SIZE)
        k = apply_rotation(kp, cos_rows, sin_rows).astype(BF16)
        v = mm(first_normed, value_weight, ((1,), (0,))).astype(BF16)
        v = v.reshape(rows, kv_local, HEAD_SIZE)
        blocks = rows // QBLK

        def block_scores(block):
            start = block * QBLK
            length = start + QBLK
            scores = (
                jnp.einsum(
                    "qgrd,kgd->grqk", q[start:length], k[:length], preferred_element_type=F32
                )
                * scale
            )
            visible = allowed(
                piece_start[0],
                piece_kind[0],
                start + jnp.arange(QBLK, dtype=jnp.int32),
                jnp.arange(length, dtype=jnp.int32),
            )
            return jnp.where(visible[None, None], scores, negative)

        outs, totals = [], []
        for block in range(blocks):
            scores = block_scores(block)
            top = jnp.max(scores, axis=-1, keepdims=True)
            total = top + jnp.log(jnp.sum(jnp.exp(scores - top), axis=-1, keepdims=True))
            probs = jnp.exp(scores - total).astype(BF16)
            length = (block + 1) * QBLK
            res = jnp.einsum("grqk,kgd->qgrd", probs, v[:length], preferred_element_type=F32)
            outs.append(res.astype(BF16))
            totals.append(total)
        head_out = jnp.concatenate(outs, axis=0).reshape(rows, q_local * HEAD_SIZE)
        mine = my_half(head_out)
        other = lax.dynamic_slice_in_dim(head_out, (1 - core) * half, half, 0)
        chip_heads = jnp.concatenate([mine, lax.ppermute(other, "tensor", CORE_PAIRS)], axis=1)
        all_heads = jnp.concatenate([chip_heads, lax.ppermute(chip_heads, "tensor", X_PAIRS)], axis=1)
        mid = my_half(resid_in) + mm(all_heads, all_output, ((1,), (0,)))
        inv_two = lax.rsqrt(jnp.mean(mid * mid, axis=1, keepdims=True) + epsilon)
        normed_half = (mid * inv_two * gain_ffn).astype(BF16)
        normed = share_half(normed_half, core)

        expert_ids = jnp.arange(E, dtype=jnp.int32)
        picked = jnp.any(choices[:, :, None] == expert_ids[None, None, :], axis=1)
        ranks = place_order[0]
        earlier = (ranks[None, :] < ranks[:, None]).astype(BF16)
        slot = mm(earlier, picked.astype(BF16), ((1,), (0,)))
        kept = (picked & (slot < CAP)).astype(F32)
        logits = mm(normed, router, ((1,), (0,)))
        logits = jnp.where(picked, logits, negative)
        gates = jax.nn.softmax(logits, axis=1)
        gates = jnp.where(picked, gates, 0.0)
        slot_gate = gates * kept

        piece = width // ways
        ff = w_gate.shape[2]
        plain = bits_of(ways)
        turned = plain[1:] + plain[:1]
        by_quad = slot_gate.reshape(rows, E // QUAD, QUAD).transpose(1, 0, 2)
        shared = (normed, normed.T, cotangent, cotangent.T, by_quad, w_gate, w_up, w_down)
        dg_one, norm_part, moe_part, keeps, sends = run_experts(0, (plain,), ways, *shared, None)
        orders = (plain, turned, plain, plain)
        dg_two, norm_part, moe_part, more_keeps, more_sends = run_experts(
            1, orders[1:], ways, *shared, (norm_part, moe_part)
        )
        keeps, sends = tuple(keeps) + tuple(more_keeps), tuple(sends) + tuple(more_sends)
        parts = [halve(keeps[c], sends[c], ways, orders[c]) for c in range(E // QUAD)]
        quads = jnp.stack(parts)
        gate_up = quads[:, :, : 2 * QUAD * ff].reshape(E // QUAD, piece, QUAD, 2, ff)
        gate_up = gate_up.transpose(3, 0, 2, 1, 4).reshape(2, E, piece, ff)
        sent_down = quads[:, :, 2 * QUAD * ff :].reshape(E // QUAD, piece, QUAD, ff)
        sent_down = sent_down.transpose(0, 2, 3, 1).reshape(E, ff, piece)
        grad_gate_part = (dg_one[:, :E] + dg_two[:, :E]) * kept

        norm_half = reduce_half(norm_part, core)
        dg_half = reduce_half(grad_gate_part, core)
        output = share_half((mid + reduce_half(moe_part, core)).astype(BF16), core)
        gates_half = my_half(gates)
        dz = gates_half * (dg_half - jnp.sum(gates_half * dg_half, axis=1, keepdims=True))
        dlg = dz.astype(BF16)
        grad_norm = norm_half + mm(dlg, router, ((1,), (1,)))
        grad_router = mm(dlg, normed_half, ((0,), (0,)))
        grad_gain_ffn = jnp.sum(grad_norm * mid * inv_two, axis=0)
        scaled = gain_ffn * grad_norm
        grad_mid = (
            my_half(cotangent).astype(F32)
            + inv_two * scaled
            - mid * inv_two**3 * jnp.mean(scaled * mid, axis=1, keepdims=True)
        )
        grad_attn = share_half(grad_mid.astype(BF16), core)
        grad_output = mm(grad_attn, head_out, ((0,), (0,)))
        grad_heads = mm(grad_attn, w_output, ((1,), (1,))).astype(BF16)
        grad_heads = grad_heads.reshape(rows, kv_local, group, HEAD_SIZE)
        query_parts = []
        grad_k = jnp.zeros((rows, kv_local, HEAD_SIZE), F32)
        grad_v = jnp.zeros((rows, kv_local, HEAD_SIZE), F32)
        for block in range(blocks):
            scores = block_scores(block)
            start = block * QBLK
            length = start + QBLK
            probs = jnp.exp(scores - totals[block])
            dob = grad_heads[start:length]
            dp = jnp.einsum("qgrd,kgd->grqk", dob, v[:length], preferred_element_type=F32)
            delta = jnp.sum(probs * dp, axis=-1, keepdims=True)
            ds = (probs * (dp - delta)).astype(BF16)
            query_parts.append(
                jnp.einsum("grqk,kgd->qgrd", ds, k[:length], preferred_element_type=F32) * scale
            )
            dk = jnp.einsum("grqk,qgrd->kgd", ds, q[start:length], preferred_element_type=F32)
            dv = jnp.einsum("grqk,qgrd->kgd", probs.astype(BF16), dob, preferred_element_type=F32)
            pad = ((0, rows - length), (0, 0), (0, 0))
            grad_k = grad_k + jnp.pad(dk * scale, pad)
            grad_v = grad_v + jnp.pad(dv, pad)
        grad_q = jnp.concatenate(query_parts, axis=0).reshape(rows, q_local, HEAD_SIZE)
        dqp = unrotate(grad_q, cos_rows, sin_rows).astype(BF16).reshape(rows, -1)
        dkp = unrotate(grad_k, cos_rows, sin_rows).astype(BF16).reshape(rows, -1)
        dvb = grad_v.astype(BF16).reshape(rows, -1)
        grad_qkv = jnp.concatenate([dqp, dkp, dvb], axis=1)
        w_qkv = jnp.concatenate([w_query, key_weight, value_weight], axis=1)
        grad_wide = mm(first_normed, grad_qkv, ((0,), (0,)))
        attn_grads = jnp.concatenate([grad_wide, grad_output], axis=1).astype(BF16)
        sent_attn = scatter_sum(attn_grads.reshape(ways, piece, -1), ways, plain)
        nq, nk = w_query.shape[1], key_weight.shape[1]
        normed_one_part = mm(grad_qkv, w_qkv, ((1,), (1,)))
        grad_gain_attn = jnp.sum(normed_one_part * resid_in * inv_one, axis=0)
        norm_one_half = reduce_half(normed_one_part, core)
        x_half = my_half(resid_in)
        inv_half = my_half(inv_one)
        scaled_one = gain_attn * norm_one_half
        input_half = (
            grad_mid
            + inv_half * scaled_one
            - x_half * inv_half**3 * jnp.mean(scaled_one * x_half, axis=1, keepdims=True)
        ).astype(BF16)
        input_grad = share_half(input_half, core)
        first_chip = (lax.axis_index("tensor") < 2).astype(F32)
        row_sums = jnp.concatenate([grad_gain_ffn[None], grad_router], axis=0) * first_chip
        small = jnp.concatenate([grad_gain_attn[None], row_sums], axis=0)
        small = small + lax.ppermute(small, "tensor", CORE_PAIRS)
        small = small + lax.ppermute(small, "tensor", X_PAIRS)
        count = small.shape[0]
        small = scatter_sum(small.reshape(count, ways, piece).transpose(1, 0, 2), ways, plain)
        return (
            output,
            input_grad,
            sent_attn[:, :nq],
            sent_attn[:, nq : nq + nk],
            sent_attn[:, nq + nk : nq + 2 * nk],
            sent_attn[:, nq + 2 * nk :].T,
            small[0],
            small[1],
            small[2:].T,
            gate_up[0],
            gate_up[1],
            sent_down,
        )

    return body


def solution(mesh):
    return jax.shard_map(
        make_body(mesh.shape["dp"]),
        mesh=mesh,
        in_specs=(
            P("dp", None),
            P(None, "tensor"),
            P(None, "tensor"),
            P(None, "tensor"),
            P("tensor", None),
            P(),
            P(),
            P(),
            P(None, None, "tensor"),
            P(None, None, "tensor"),
            P(None, "tensor", None),
            P("dp", None),
            P("dp", None),
            P("dp", None),
            P("dp", None),
            P("dp", None),
        ),
        out_specs=(
            P("dp", None),
            P("dp", None),
            P("dp", "tensor"),
            P("dp", "tensor"),
            P("dp", "tensor"),
            P("tensor", "dp"),
            P("dp"),
            P("dp"),
            P("dp", None),
            P(None, "dp", "tensor"),
            P(None, "dp", "tensor"),
            P(None, "tensor", "dp"),
        ),
        check_vma=False,
    )
```

```python
import functools

import jax
import jax.numpy as jnp
from jax import lax
from jax.experimental import pallas as pl
from jax.experimental.pallas import tpu as pltpu
from jax.sharding import PartitionSpec as P


HEAD_SIZE = 64
E = 16
PIECE = 256
QBLK = 512
CAP = 640

epsilon = 1e-06
negative = -1e30
F32 = jnp.float32
BF16 = jnp.bfloat16


def mm(left, right, dims):
    return lax.dot_general(left, right, (dims, ((), ())), preferred_element_type=F32)


def rope_tables(sequence_length):
    half_width = HEAD_SIZE // 2
    frequency = 10000.0 ** (-(jnp.arange(half_width, dtype=F32) * 2.0 / HEAD_SIZE))
    angles = jnp.arange(sequence_length, dtype=F32)[:, None] * frequency[None, :]
    return (jnp.cos(angles), jnp.sin(angles))


def apply_rotation(values, cosine_table, sine_values):
    half_width = HEAD_SIZE // 2
    first = values[..., :half_width]
    second = values[..., half_width:]
    cos_part = cosine_table[:, None, :]
    sin_part = sine_values[:, None, :]
    return jnp.concatenate(
        [first * cos_part - second * sin_part, second * cos_part + first * sin_part], axis=-1
    )


def unrotate(grads, cosine_table, sine_values):
    return apply_rotation(grads, cosine_table, -sine_values)


def allowed(starts, kind_row, row_pos, col_pos):
    ends = starts + PIECE
    inside_row = (
        (kind_row[None, :] == 1)
        & (row_pos[:, None] >= starts[None, :])
        & (row_pos[:, None] < ends[None, :])
    )
    inside_col = (
        (kind_row[None, :] == 1)
        & (col_pos[:, None] >= starts[None, :])
        & (col_pos[:, None] < ends[None, :])
    )
    same_piece = jnp.any(inside_row[:, None, :] & inside_col[None, :, :], axis=-1)
    return (col_pos[None, :] <= row_pos[:, None]) | same_piece


CORE_PAIRS = [(i, i ^ 1) for i in range(4)]
X_PAIRS = [(i, i ^ 2) for i in range(4)]


def reduce_half(part, core):
    half = part.shape[0] // 2
    mine = lax.dynamic_slice_in_dim(part, core * half, half, 0)
    other = lax.dynamic_slice_in_dim(part, (1 - core) * half, half, 0).astype(BF16)
    got = lax.ppermute(other, "tensor", CORE_PAIRS)
    total = (mine + got.astype(F32)).astype(BF16)
    far = lax.ppermute(total, "tensor", X_PAIRS)
    return total, far


def share_half(half_rows, core):
    got = lax.ppermute(half_rows, "tensor", CORE_PAIRS)
    pair = jnp.stack([jnp.where(core == 0, half_rows, got), jnp.where(core == 0, got, half_rows)])
    return pair.reshape((2 * half_rows.shape[0],) + half_rows.shape[1:])


def bits_of(ways):
    return tuple(range(ways.bit_length() - 1))


def flip(array, ways, bit):
    return lax.ppermute(array, "dp", [(i, i ^ (1 << bit)) for i in range(ways)])


def halve(keep, send, ways, order):
    got = flip(send, ways, order[0])
    for bit in order[1:]:
        half = keep.shape[0] // 2
        to_send = (keep[half:].astype(F32) + got[half:].astype(F32)).astype(keep.dtype)
        keep = (keep[:half].astype(F32) + got[:half].astype(F32)).astype(keep.dtype)
        got = flip(to_send, ways, bit)
    return keep, got


def scatter_sums(arrays, ways, order):
    me = lax.axis_index("dp")
    count = len(order)
    current = [blocks.reshape((2,) * count + blocks.shape[1:]) for blocks in arrays]
    left = list(reversed(range(count)))
    for bit in order:
        axis = left.index(bit)
        mine_at = (me >> bit) & 1
        left.remove(bit)
        for i, blocks in enumerate(current):
            mine = lax.dynamic_index_in_dim(blocks, mine_at, axis, keepdims=False)
            other = lax.dynamic_index_in_dim(blocks, 1 - mine_at, axis, keepdims=False)
            got = flip(other, ways, bit)
            total = mine.astype(F32) + got.astype(F32)
            current[i] = total.astype(blocks.dtype) if left else total
    return current


QUAD = 4
ROWS = 512


def expert_kernel(first, ways, order, carried, *refs):
    own_gate, got_gate, own_x, got_x, dy_hbm, wg_hbm, wu_hbm, wd_hbm = refs[:8]
    refs = refs[8:]
    if carried:
        xt_hbm, dyt_hbm, norm_in, moe_in, dg_ref, norm_out, moe_out, keep, send = refs[:9]
        refs = refs[9:]
    else:
        dg_ref, norm_out, moe_out, keep, send, xt_hbm, dyt_hbm = refs[:7]
        refs = refs[7:]
    x_ref, xt_ref, dy_ref, dyt_ref, wgu, wd, gu, gated, grads, norm_acc, moe_acc = refs[:11]
    gate_ref, block_sem, sem = refs[11:]
    rows, width = x_ref.shape
    ff = wg_hbm.shape[2]
    piece = width // ways
    half = ways // 2
    me = lax.axis_index("dp")

    loads = []
    for j in range(QUAD):
        gate_at = pl.ds(2 * j * ff, ff)
        up_at = pl.ds((2 * j + 1) * ff, ff)
        loads.append(pltpu.make_async_copy(wg_hbm.at[first + j], wgu.at[:, gate_at], sem.at[j]))
        loads.append(pltpu.make_async_copy(wu_hbm.at[first + j], wgu.at[:, up_at], sem.at[QUAD + j]))
    for j in range(QUAD):
        down_at = pl.ds(j * ff, ff)
        loads.append(pltpu.make_async_copy(wd_hbm.at[first + j], wd.at[down_at, :], sem.at[2 * QUAD + j]))
    core = lax.axis_index("tensor") % 2
    rows_half = rows // 2
    own_at = pl.ds(pl.multiple_of(core * rows_half, rows_half), rows_half)
    got_at = pl.ds(pl.multiple_of((1 - core) * rows_half, rows_half), rows_half)
    loads = [
        pltpu.make_async_copy(own_x, x_ref.at[own_at, :], sem.at[3 * QUAD]),
        pltpu.make_async_copy(got_x, x_ref.at[got_at, :], sem.at[3 * QUAD + 6]),
    ] + loads
    loads.append(pltpu.make_async_copy(own_gate, gate_ref.at[own_at, :], sem.at[3 * QUAD + 7]))
    loads.append(pltpu.make_async_copy(got_gate, gate_ref.at[got_at, :], sem.at[3 * QUAD + 8]))
    loads.append(pltpu.make_async_copy(dy_hbm, dy_ref, sem.at[3 * QUAD + 1]))
    for load in loads:
        load.start()
    if carried:
        load_norm = pltpu.make_async_copy(norm_in, norm_acc, sem.at[3 * QUAD + 4])
        load_moe = pltpu.make_async_copy(moe_in, moe_acc, sem.at[3 * QUAD + 5])
        load_xt = pltpu.make_async_copy(xt_hbm, xt_ref, sem.at[3 * QUAD + 2])
        load_dyt = pltpu.make_async_copy(dyt_hbm, dyt_ref, sem.at[3 * QUAD + 3])
        for load in (load_norm, load_moe, load_xt, load_dyt):
            load.start()
    dg_ref[...] = jnp.zeros_like(dg_ref)
    for load in loads:
        load.wait()
    lane = lax.broadcasted_iota(jnp.int32, (ROWS, dg_ref.shape[1]), 1)

    def hidden_rows(i, _):
        at = pl.ds(pl.multiple_of(i * ROWS, ROWS), ROWS)
        au = mm(x_ref[at, :], wgu[...], ((1,), (0,)))
        down = mm(dy_ref[at, :], wd[...], ((1,), (1,)))
        gate_rows = gate_ref[at, :]
        dg = dg_ref[at, :]
        for j in range(QUAD):
            pre = au[:, 2 * j * ff : (2 * j + 1) * ff]
            up = au[:, (2 * j + 1) * ff : (2 * j + 2) * ff]
            back = down[:, j * ff : (j + 1) * ff]
            gate = gate_rows[:, first + j : first + j + 1]
            sigmoid = 1.0 / (1.0 + jnp.exp(-pre))
            act = pre * sigmoid
            hidden = act * up
            gated[at, j * ff : (j + 1) * ff] = (gate * hidden).astype(BF16)
            row = jnp.sum(hidden * back, axis=1, keepdims=True)
            dg = jnp.where(lane == first + j, row, dg)
            back = gate * back
            slope = sigmoid * (1.0 + pre * (1.0 - sigmoid))
            gu[at, 2 * j * ff : (2 * j + 1) * ff] = (back * up * slope).astype(BF16)
            gu[at, (2 * j + 1) * ff : (2 * j + 2) * ff] = (back * act).astype(BF16)
        dg_ref[at, :] = dg
        return 0

    lax.fori_loop(0, rows // ROWS, hidden_rows, 0)
    if carried:
        load_norm.wait()
        load_moe.wait()

    def data_rows(i, _):
        at = pl.ds(pl.multiple_of(i * ROWS, ROWS), ROWS)
        norm = mm(gu[at, :], wgu[...], ((1,), (1,)))
        moe = mm(gated[at, :], wd[...], ((1,), (0,)))
        if carried:
            norm_acc[at, :] += norm
            moe_acc[at, :] += moe
        else:
            norm_acc[at, :] = norm
            moe_acc[at, :] = moe
            xt_ref[:, at] = x_ref[at, :].T
            dyt_ref[:, at] = dy_ref[at, :].T
        return 0

    lax.fori_loop(0, rows // ROWS, data_rows, 0)
    save_norm = pltpu.make_async_copy(norm_acc, norm_out, sem.at[3 * QUAD + 4])
    save_moe = pltpu.make_async_copy(moe_acc, moe_out, sem.at[3 * QUAD + 5])
    save_norm.start()
    save_moe.start()
    if carried:
        load_xt.wait()
        load_dyt.wait()
    else:
        save_xt = pltpu.make_async_copy(xt_ref, xt_hbm, sem.at[3 * QUAD + 2])
        save_dyt = pltpu.make_async_copy(dyt_ref, dyt_hbm, sem.at[3 * QUAD + 3])
        save_xt.start()
        save_dyt.start()

    def grad_rows(i, _):
        at = pl.ds(pl.multiple_of(i * ROWS, ROWS), ROWS)
        grads[at, : 2 * QUAD * ff] = mm(xt_ref[at, :], gu[...], ((1,), (0,))).astype(BF16)
        grads[at, 2 * QUAD * ff :] = mm(dyt_ref[at, :], gated[...], ((1,), (0,))).astype(BF16)
        return 0

    lax.fori_loop(0, width // ROWS, grad_rows, 0)
    copies = []
    for slot in range(ways):
        dest = 0
        for place, bit in enumerate(order):
            own = (slot >> (len(order) - 1 - place)) & 1
            dest = dest + ((me // (1 << bit) + own) % 2) * (1 << bit)
        block = grads.at[pl.ds(pl.multiple_of(dest * piece, piece), piece), :]
        target = keep.at[slot] if slot < half else send.at[slot - half]
        copies.append(pltpu.make_async_copy(block, target, block_sem.at[slot]))
    for copy in copies:
        copy.start()
    for copy in copies:
        copy.wait()
    save_norm.wait()
    save_moe.wait()
    if not carried:
        save_xt.wait()
        save_dyt.wait()


def run_experts(quad, order, ways, own_gate, got_gate, own_x, got_x, dy, w_gate, w_up, w_down, carry):
    rows, width = dy.shape
    ff = w_gate.shape[2]
    piece = width // ways
    any_space = pl.BlockSpec(memory_space=pl.ANY)
    vmem = pl.BlockSpec(memory_space=pltpu.VMEM)
    wide = 3 * QUAD * ff
    block = jax.ShapeDtypeStruct((ways // 2, piece, wide), BF16)
    total = jax.ShapeDtypeStruct((rows, width), F32)
    turned = jax.ShapeDtypeStruct((width, rows), BF16)
    flops = 2 * 9 * QUAD * rows * width * ff
    moved = QUAD * width * ff * 12 + rows * width * 8 + rows * width * 16
    return pl.pallas_call(
        functools.partial(expert_kernel, quad * QUAD, ways, order, carry is not None),
        out_shape=(jax.ShapeDtypeStruct((rows, 128), F32), total, total, block, block)
        + ((turned, turned) if carry is None else ()),
        in_specs=[any_space] * (8 if carry is None else 12),
        out_specs=(vmem,) + (any_space,) * (6 if carry is None else 4),
        scratch_shapes=[
            pltpu.VMEM((rows, width), BF16),
            pltpu.VMEM((width, rows), BF16),
            pltpu.VMEM((rows, width), BF16),
            pltpu.VMEM((width, rows), BF16),
            pltpu.VMEM((width, 2 * QUAD * ff), BF16),
            pltpu.VMEM((QUAD * ff, width), BF16),
            pltpu.VMEM((rows, 2 * QUAD * ff), BF16),
            pltpu.VMEM((rows, QUAD * ff), BF16),
            pltpu.VMEM((width, wide), BF16),
            pltpu.VMEM((rows, width), F32),
            pltpu.VMEM((rows, width), F32),
            pltpu.VMEM((rows, E), F32),
            pltpu.SemaphoreType.DMA((ways,)),
            pltpu.SemaphoreType.DMA((3 * QUAD + 9,)),
        ],
        compiler_params=pltpu.CompilerParams(vmem_limit_bytes=44 << 20),
        cost_estimate=pl.CostEstimate(
            flops=flops, bytes_accessed=moved, transcendentals=QUAD * rows * ff
        ),
    )(own_gate, got_gate, own_x, got_x, dy, w_gate, w_up, w_down, *(carry if carry is not None else ()))


def unpack_kernel(quads, *refs):
    keeps, gots = refs[:quads], refs[quads : 2 * quads]
    gate_ref, up_ref, down_ref = refs[2 * quads :]
    ff = gate_ref.shape[2]
    for quad in range(quads):
        for j in range(QUAD):
            def part(first):
                at = slice(first * ff, (first + 1) * ff)
                return keeps[quad][0, :, at].astype(F32) + gots[quad][0, :, at].astype(F32)

            gate_ref[quad * QUAD + j] = part(2 * j)
            up_ref[quad * QUAD + j] = part(2 * j + 1)
            down_ref[quad * QUAD + j] = part(2 * QUAD + j).T


def unpack(keeps, gots, ff):
    piece = keeps[0].shape[1]
    experts = QUAD * len(keeps)
    vmem = pl.BlockSpec(memory_space=pltpu.VMEM)
    flat = jax.ShapeDtypeStruct((experts, piece, ff), F32)
    return pl.pallas_call(
        functools.partial(unpack_kernel, len(keeps)),
        out_shape=(flat, flat, jax.ShapeDtypeStruct((experts, ff, piece), F32)),
        in_specs=[vmem] * (2 * len(keeps)),
        out_specs=(vmem,) * 3,
        cost_estimate=pl.CostEstimate(
            flops=experts * piece * ff * 3, bytes_accessed=experts * piece * ff * 24, transcendentals=0
        ),
        name="unpack",
    )(*keeps, *gots)


def make_body(ways):
    def body(
        tokens,
        w_query,
        key_weight,
        value_weight,
        w_output,
        gain_attn,
        gain_ffn,
        router,
        w_gate,
        w_up,
        w_down,
        piece_start,
        piece_kind,
        choices,
        place_order,
        cotangent,
    ):
        rows = tokens.shape[0]
        half = rows // 2
        width = tokens.shape[1]
        kv_local = key_weight.shape[1] // HEAD_SIZE
        q_local = w_query.shape[1] // HEAD_SIZE
        ff = w_gate.shape[2]
        group = q_local // kv_local
        scale = HEAD_SIZE ** (-0.5)
        core = lax.axis_index("tensor") % 2

        def my_half(array):
            return lax.dynamic_slice_in_dim(array, core * half, half, 0)

        from_x = lax.ppermute(w_output, "tensor", X_PAIRS)
        near = jnp.stack([w_output, from_x])
        far = lax.ppermute(near, "tensor", CORE_PAIRS)
        all_output = jnp.concatenate([w_output, far[0], from_x, far[1]], axis=0)
        resid_in = tokens.astype(F32)
        inv_one = lax.rsqrt(jnp.mean(resid_in * resid_in, axis=1, keepdims=True) + epsilon)
        first_normed = (resid_in * inv_one * gain_attn).astype(BF16)
        cos_rows, sin_rows = rope_tables(rows)
        qp = mm(first_normed, w_query, ((1,), (0,))).reshape(rows, q_local, HEAD_SIZE)
        q = apply_rotation(qp, cos_rows, sin_rows).astype(BF16)
        q = q.reshape(rows, kv_local, group, HEAD_SIZE)
        kp = mm(first_normed, key_weight, ((1,), (0,))).reshape(rows, kv_local, HEAD_SIZE)
        k = apply_rotation(kp, cos_rows, sin_rows).astype(BF16)
        v = mm(first_normed, value_weight, ((1,), (0,))).astype(BF16)
        v = v.reshape(rows, kv_local, HEAD_SIZE)
        blocks = rows // QBLK

        def block_scores(block):
            start = block * QBLK
            length = start + QBLK
            scores = (
                jnp.einsum(
                    "qgrd,kgd->grqk", q[start:length], k[:length], preferred_element_type=F32
                )
                * scale
            )
            visible = allowed(
                piece_start[0],
                piece_kind[0],
                start + jnp.arange(QBLK, dtype=jnp.int32),
                jnp.arange(length, dtype=jnp.int32),
            )
            return jnp.where(visible[None, None], scores, negative)

        outs, totals = [], []
        for block in range(blocks):
            scores = block_scores(block)
            top = jnp.max(scores, axis=-1, keepdims=True)
            total = top + jnp.log(jnp.sum(jnp.exp(scores - top), axis=-1, keepdims=True))
            probs = jnp.exp(scores - total).astype(BF16)
            length = (block + 1) * QBLK
            res = jnp.einsum("grqk,kgd->qgrd", probs, v[:length], preferred_element_type=F32)
            outs.append(res.astype(BF16))
            totals.append(total)
        head_out = jnp.concatenate(outs, axis=0).reshape(rows, q_local * HEAD_SIZE)
        mine = my_half(head_out)
        other = lax.dynamic_slice_in_dim(head_out, (1 - core) * half, half, 0)
        chip_heads = jnp.concatenate([mine, lax.ppermute(other, "tensor", CORE_PAIRS)], axis=1)
        far_heads = lax.ppermute(chip_heads, "tensor", X_PAIRS)
        all_heads = jnp.concatenate([chip_heads, far_heads], axis=1)
        mid = my_half(resid_in) + mm(all_heads, all_output, ((1,), (0,)))
        inv_two = lax.rsqrt(jnp.mean(mid * mid, axis=1, keepdims=True) + epsilon)
        normed_half = (mid * inv_two * gain_ffn).astype(BF16)
        normed_far = lax.ppermute(normed_half, "tensor", CORE_PAIRS)

        expert_ids = jnp.arange(E, dtype=jnp.int32)
        picked = jnp.any(choices[:, :, None] == expert_ids[None, None, :], axis=1)
        ranks = place_order[0]
        earlier = (ranks[None, :] < ranks[:, None]).astype(BF16)
        slot = mm(earlier, picked.astype(BF16), ((1,), (0,)))
        kept = (picked & (slot < CAP)).astype(F32)
        picked_half = my_half(picked.astype(F32))
        kept_half = my_half(kept)
        logits = mm(normed_half, router, ((1,), (0,)))
        logits = jnp.where(picked_half > 0, logits, negative)
        gates_half = jax.nn.softmax(logits, axis=1)
        gates_half = jnp.where(picked_half > 0, gates_half, 0.0)
        slot_gate = gates_half * kept_half
        slot_gate_far = lax.ppermute(slot_gate, "tensor", CORE_PAIRS)

        piece = width // ways
        ff = w_gate.shape[2]
        plain = bits_of(ways)
        turned = plain[1:] + plain[:1]
        shared = (slot_gate, slot_gate_far, normed_half, normed_far, cotangent, w_gate, w_up, w_down)
        orders = (plain, turned, plain, plain)
        carry = None
        dg_parts, keeps, gots = [], [], []
        for quad in range(E // QUAD):
            result = run_experts(quad, orders[quad], ways, *shared, carry)
            dg_part, norm_part, moe_part, keep, send = result[:5]
            carry = (result[5:] if quad == 0 else carry[:2]) + (norm_part, moe_part)
            dg_parts.append(dg_part[:, quad * QUAD : (quad + 1) * QUAD])
            keep, got = halve(keep, send, ways, orders[quad])
            keeps.append(keep)
            gots.append(got)
        sent_gate, sent_up, sent_down = unpack(keeps, gots, ff)
        grad_gate_part = jnp.concatenate(dg_parts, axis=1) * kept

        norm_near, norm_far = reduce_half(norm_part, core)
        norm_half = norm_near.astype(F32) + norm_far.astype(F32)
        dg_near, dg_far = reduce_half(grad_gate_part, core)
        dg_half = dg_near.astype(F32) + dg_far.astype(F32)
        moe_near, moe_far = reduce_half(moe_part, core)
        dz = gates_half * (dg_half - jnp.sum(gates_half * dg_half, axis=1, keepdims=True))
        dlg = dz.astype(BF16)
        grad_norm = norm_half + mm(dlg, router, ((1,), (1,)))
        grad_router = mm(dlg, normed_half, ((0,), (0,)))
        grad_gain_ffn = jnp.sum(grad_norm * mid * inv_two, axis=0)
        scaled = gain_ffn * grad_norm
        grad_mid = (
            my_half(cotangent).astype(F32)
            + inv_two * scaled
            - mid * inv_two**3 * jnp.mean(scaled * mid, axis=1, keepdims=True)
        )
        grad_attn = share_half(grad_mid.astype(BF16), core)
        grad_output = mm(grad_attn, head_out, ((0,), (0,)))
        grad_heads = mm(grad_attn, w_output, ((1,), (1,))).astype(BF16)
        grad_heads = grad_heads.reshape(rows, kv_local, group, HEAD_SIZE)
        query_parts = []
        grad_k = jnp.zeros((rows, kv_local, HEAD_SIZE), F32)
        grad_v = jnp.zeros((rows, kv_local, HEAD_SIZE), F32)
        for block in range(blocks):
            scores = block_scores(block)
            start = block * QBLK
            length = start + QBLK
            probs = jnp.exp(scores - totals[block])
            dob = grad_heads[start:length]
            dp = jnp.einsum("qgrd,kgd->grqk", dob, v[:length], preferred_element_type=F32)
            delta = jnp.sum(probs * dp, axis=-1, keepdims=True)
            ds = (probs * (dp - delta)).astype(BF16)
            query_parts.append(
                jnp.einsum("grqk,kgd->qgrd", ds, k[:length], preferred_element_type=F32) * scale
            )
            dk = jnp.einsum("grqk,qgrd->kgd", ds, q[start:length], preferred_element_type=F32)
            dv = jnp.einsum("grqk,qgrd->kgd", probs.astype(BF16), dob, preferred_element_type=F32)
            pad = ((0, rows - length), (0, 0), (0, 0))
            grad_k = grad_k + jnp.pad(dk * scale, pad)
            grad_v = grad_v + jnp.pad(dv, pad)
        grad_q = jnp.concatenate(query_parts, axis=0).reshape(rows, q_local, HEAD_SIZE)
        dqp = unrotate(grad_q, cos_rows, sin_rows).astype(BF16).reshape(rows, -1)
        dkp = unrotate(grad_k, cos_rows, sin_rows).astype(BF16).reshape(rows, -1)
        dvb = grad_v.astype(BF16).reshape(rows, -1)
        grad_qkv = jnp.concatenate([dqp, dkp, dvb], axis=1)
        w_qkv = jnp.concatenate([w_query, key_weight, value_weight], axis=1)
        grad_wide = mm(first_normed, grad_qkv, ((0,), (0,)))
        moe_far, grad_wide = lax.optimization_barrier((moe_far, grad_wide))
        output = (mid + (moe_near.astype(F32) + moe_far.astype(F32))).astype(BF16)
        output = share_half(output, core)
        attn_grads = jnp.concatenate([grad_wide, grad_output], axis=1).astype(BF16)
        attn_grads = attn_grads.reshape(ways, piece, -1)
        nq, nk = w_query.shape[1], key_weight.shape[1]
        normed_one_part = mm(grad_qkv, w_qkv, ((1,), (1,)))
        grad_gain_attn = jnp.sum(normed_one_part * resid_in * inv_one, axis=0)
        last_near, last_far = reduce_half(normed_one_part, core)
        norm_one_half = last_near.astype(F32) + last_far.astype(F32)
        x_half = my_half(resid_in)
        inv_half = my_half(inv_one)
        scaled_one = gain_attn * norm_one_half
        input_half = (
            grad_mid
            + inv_half * scaled_one
            - x_half * inv_half**3 * jnp.mean(scaled_one * x_half, axis=1, keepdims=True)
        ).astype(BF16)
        input_grad = share_half(input_half, core)
        first_chip = (lax.axis_index("tensor") < 2).astype(F32)
        row_sums = jnp.concatenate([grad_gain_ffn[None], grad_router], axis=0) * first_chip
        small = jnp.concatenate([grad_gain_attn[None], row_sums], axis=0)
        small = small + lax.ppermute(small, "tensor", CORE_PAIRS)
        small = small + lax.ppermute(small, "tensor", X_PAIRS)
        count = small.shape[0]
        small = small.reshape(count, ways, piece).transpose(1, 0, 2)
        sent_attn, small = scatter_sums((attn_grads, small), ways, plain)
        return (
            output,
            input_grad,
            sent_attn[:, :nq],
            sent_attn[:, nq : nq + nk],
            sent_attn[:, nq + nk : nq + 2 * nk],
            sent_attn[:, nq + 2 * nk :].T,
            small[0],
            small[1],
            small[2:].T,
            sent_gate,
            sent_up,
            sent_down,
        )

    return body


def solution(mesh):
    body = make_body(mesh.shape["dp"])

    return jax.shard_map(
        body,
        mesh=mesh,
        in_specs=(
            P("dp", None),
            P(None, "tensor"),
            P(None, "tensor"),
            P(None, "tensor"),
            P("tensor", None),
            P(),
            P(),
            P(),
            P(None, None, "tensor"),
            P(None, None, "tensor"),
            P(None, "tensor", None),
            P("dp", None),
            P("dp", None),
            P("dp", None),
            P("dp", None),
            P("dp", None),
        ),
        out_specs=(
            P("dp", None),
            P("dp", None),
            P("dp", "tensor"),
            P("dp", "tensor"),
            P("dp", "tensor"),
            P("tensor", "dp"),
            P("dp"),
            P("dp"),
            P("dp", None),
            P(None, "dp", "tensor"),
            P(None, "dp", "tensor"),
            P(None, "tensor", "dp"),
        ),
        check_vma=False,
    )
```

```python
import functools

import jax
import jax.numpy as jnp
import numpy as np
from jax import lax
from jax.experimental import pallas as pl
from jax.experimental.pallas import tpu as pltpu
from jax.sharding import PartitionSpec as P


HEAD_SIZE = 64
E = 16
PIECE = 256
QBLK = 512
CAP = 640

epsilon = 1e-06
negative = -1e30
F32 = jnp.float32
BF16 = jnp.bfloat16


def mm(left, right, dims):
    return lax.dot_general(left, right, (dims, ((), ())), preferred_element_type=F32)


CORE_PAIRS = [(i, i ^ 1) for i in range(4)]
X_PAIRS = [(i, i ^ 2) for i in range(4)]


def reduce_half(part, core):
    half = part.shape[0] // 2
    mine = lax.dynamic_slice_in_dim(part, core * half, half, 0)
    other = lax.dynamic_slice_in_dim(part, (1 - core) * half, half, 0).astype(BF16)
    got = lax.ppermute(other, "tensor", CORE_PAIRS)
    total = (mine + got.astype(F32)).astype(BF16)
    far = lax.ppermute(total, "tensor", X_PAIRS)
    return total, far


def share_half(half_rows, core):
    got = lax.ppermute(half_rows, "tensor", CORE_PAIRS)
    pair = jnp.stack([jnp.where(core == 0, half_rows, got), jnp.where(core == 0, got, half_rows)])
    return pair.reshape((2 * half_rows.shape[0],) + half_rows.shape[1:])


def bits_of(ways):
    return tuple(range(ways.bit_length() - 1))


def flip(array, ways, bit):
    return lax.ppermute(array, "dp", [(i, i ^ (1 << bit)) for i in range(ways)])


def halve(keep, send, ways, order):
    got = flip(send, ways, order[0])
    for bit in order[1:]:
        half = keep.shape[0] // 2
        to_send = (keep[half:].astype(F32) + got[half:].astype(F32)).astype(keep.dtype)
        keep = (keep[:half].astype(F32) + got[:half].astype(F32)).astype(keep.dtype)
        got = flip(to_send, ways, bit)
    return keep, got


def scatter_sums(arrays, ways, order):
    me = lax.axis_index("dp")
    count = len(order)
    current = [blocks.reshape((2,) * count + blocks.shape[1:]) for blocks in arrays]
    left = list(reversed(range(count)))
    for bit in order:
        axis = left.index(bit)
        mine_at = (me >> bit) & 1
        left.remove(bit)
        for i, blocks in enumerate(current):
            mine = lax.dynamic_index_in_dim(blocks, mine_at, axis, keepdims=False)
            other = lax.dynamic_index_in_dim(blocks, 1 - mine_at, axis, keepdims=False)
            got = flip(other, ways, bit)
            total = mine.astype(F32) + got.astype(F32)
            current[i] = total.astype(blocks.dtype) if left else total
    return current


QUAD = 4
ROWS = 512


def expert_kernel(first, ways, order, carried, *refs):
    own_gate, got_gate, own_x, got_x, dy_hbm, wg_hbm, wu_hbm, wd_hbm = refs[:8]
    refs = refs[8:]
    if carried:
        xt_hbm, dyt_hbm, norm_in, moe_in, dg_ref, norm_out, moe_out, keep, send = refs[:9]
        refs = refs[9:]
    else:
        dg_ref, norm_out, moe_out, keep, send, xt_hbm, dyt_hbm = refs[:7]
        refs = refs[7:]
    x_ref, xt_ref, dy_ref, dyt_ref, wgu, wd, gu, gated, grads, norm_acc, moe_acc = refs[:11]
    gate_ref, block_sem, sem = refs[11:]
    rows, width = x_ref.shape
    ff = wg_hbm.shape[2]

    loads = []
    for j in range(QUAD):
        gate_at = pl.ds(2 * j * ff, ff)
        up_at = pl.ds((2 * j + 1) * ff, ff)
        loads.append(pltpu.make_async_copy(wg_hbm.at[first + j], wgu.at[:, gate_at], sem.at[j]))
        loads.append(pltpu.make_async_copy(wu_hbm.at[first + j], wgu.at[:, up_at], sem.at[QUAD + j]))
    for j in range(QUAD):
        down_at = pl.ds(j * ff, ff)
        loads.append(pltpu.make_async_copy(wd_hbm.at[first + j], wd.at[down_at, :], sem.at[2 * QUAD + j]))
    core = lax.axis_index("tensor") % 2
    rows_half = rows // 2
    own_at = pl.ds(pl.multiple_of(core * rows_half, rows_half), rows_half)
    got_at = pl.ds(pl.multiple_of((1 - core) * rows_half, rows_half), rows_half)
    loads = [
        pltpu.make_async_copy(own_x, x_ref.at[own_at, :], sem.at[3 * QUAD]),
        pltpu.make_async_copy(got_x, x_ref.at[got_at, :], sem.at[3 * QUAD + 6]),
    ] + loads
    loads.append(pltpu.make_async_copy(own_gate, gate_ref.at[own_at, :], sem.at[3 * QUAD + 7]))
    loads.append(pltpu.make_async_copy(got_gate, gate_ref.at[got_at, :], sem.at[3 * QUAD + 8]))
    loads.append(pltpu.make_async_copy(dy_hbm, dy_ref, sem.at[3 * QUAD + 1]))
    for load in loads:
        load.start()
    if carried:
        load_norm = pltpu.make_async_copy(norm_in, norm_acc, sem.at[3 * QUAD + 4])
        load_moe = pltpu.make_async_copy(moe_in, moe_acc, sem.at[3 * QUAD + 5])
        load_xt = pltpu.make_async_copy(xt_hbm, xt_ref, sem.at[3 * QUAD + 2])
        load_dyt = pltpu.make_async_copy(dyt_hbm, dyt_ref, sem.at[3 * QUAD + 3])
        for load in (load_norm, load_moe, load_xt, load_dyt):
            load.start()
    dg_ref[...] = jnp.zeros_like(dg_ref)
    for load in loads:
        load.wait()
    lane = lax.broadcasted_iota(jnp.int32, (ROWS, dg_ref.shape[1]), 1)

    def hidden_rows(i, _):
        at = pl.ds(pl.multiple_of(i * ROWS, ROWS), ROWS)
        au = mm(x_ref[at, :], wgu[...], ((1,), (0,)))
        down = mm(dy_ref[at, :], wd[...], ((1,), (1,)))
        gate_rows = gate_ref[at, :]
        dg = dg_ref[at, :]
        for j in range(QUAD):
            pre = au[:, 2 * j * ff : (2 * j + 1) * ff]
            up = au[:, (2 * j + 1) * ff : (2 * j + 2) * ff]
            back = down[:, j * ff : (j + 1) * ff]
            gate = gate_rows[:, first + j : first + j + 1]
            sigmoid = 1.0 / (1.0 + jnp.exp(-pre))
            act = pre * sigmoid
            hidden = act * up
            gated[at, j * ff : (j + 1) * ff] = (gate * hidden).astype(BF16)
            row = jnp.sum(hidden * back, axis=1, keepdims=True)
            dg = jnp.where(lane == first + j, row, dg)
            back = gate * back
            slope = sigmoid * (1.0 + pre * (1.0 - sigmoid))
            gu[at, 2 * j * ff : (2 * j + 1) * ff] = (back * up * slope).astype(BF16)
            gu[at, (2 * j + 1) * ff : (2 * j + 2) * ff] = (back * act).astype(BF16)
        dg_ref[at, :] = dg
        return 0

    lax.fori_loop(0, rows // ROWS, hidden_rows, 0)
    if carried:
        load_norm.wait()
        load_moe.wait()

    def data_rows(i, _):
        at = pl.ds(pl.multiple_of(i * ROWS, ROWS), ROWS)
        norm = mm(gu[at, :], wgu[...], ((1,), (1,)))
        moe = mm(gated[at, :], wd[...], ((1,), (0,)))
        if carried:
            norm_acc[at, :] += norm
            moe_acc[at, :] += moe
        else:
            norm_acc[at, :] = norm
            moe_acc[at, :] = moe
            xt_ref[:, at] = x_ref[at, :].T
            dyt_ref[:, at] = dy_ref[at, :].T
        return 0

    lax.fori_loop(0, rows // ROWS, data_rows, 0)
    save_norm = pltpu.make_async_copy(norm_acc, norm_out, sem.at[3 * QUAD + 4])
    save_moe = pltpu.make_async_copy(moe_acc, moe_out, sem.at[3 * QUAD + 5])
    save_norm.start()
    save_moe.start()
    if carried:
        load_xt.wait()
        load_dyt.wait()
    else:
        save_xt = pltpu.make_async_copy(xt_ref, xt_hbm, sem.at[3 * QUAD + 2])
        save_dyt = pltpu.make_async_copy(dyt_ref, dyt_hbm, sem.at[3 * QUAD + 3])
        save_xt.start()
        save_dyt.start()

    def grad_rows(i, _):
        at = pl.ds(pl.multiple_of(i * ROWS, ROWS), ROWS)
        grads[at, : 2 * QUAD * ff] = mm(xt_ref[at, :], gu[...], ((1,), (0,))).astype(BF16)
        grads[at, 2 * QUAD * ff :] = mm(dyt_ref[at, :], gated[...], ((1,), (0,))).astype(BF16)
        return 0

    lax.fori_loop(0, width // ROWS, grad_rows, 0)
    copies = place_blocks(grads, keep, send, ways, order, block_sem)
    for copy in copies:
        copy.start()
    for copy in copies:
        copy.wait()
    save_norm.wait()
    save_moe.wait()
    if not carried:
        save_xt.wait()
        save_dyt.wait()


def run_experts(quad, order, ways, own_gate, got_gate, own_x, got_x, dy, w_gate, w_up, w_down, carry):
    rows, width = dy.shape
    ff = w_gate.shape[2]
    piece = width // ways
    any_space = pl.BlockSpec(memory_space=pl.ANY)
    vmem = pl.BlockSpec(memory_space=pltpu.VMEM)
    wide = 3 * QUAD * ff
    block = jax.ShapeDtypeStruct((ways // 2, piece, wide), BF16)
    total = jax.ShapeDtypeStruct((rows, width), F32)
    turned = jax.ShapeDtypeStruct((width, rows), BF16)
    flops = 2 * 9 * QUAD * rows * width * ff
    moved = QUAD * width * ff * 12 + rows * width * 8 + rows * width * 16
    return pl.pallas_call(
        functools.partial(expert_kernel, quad * QUAD, ways, order, carry is not None),
        out_shape=(jax.ShapeDtypeStruct((rows, 128), F32), total, total, block, block)
        + ((turned, turned) if carry is None else ()),
        in_specs=[any_space] * (8 if carry is None else 12),
        out_specs=(vmem,) + (any_space,) * (6 if carry is None else 4),
        scratch_shapes=[
            pltpu.VMEM((rows, width), BF16),
            pltpu.VMEM((width, rows), BF16),
            pltpu.VMEM((rows, width), BF16),
            pltpu.VMEM((width, rows), BF16),
            pltpu.VMEM((width, 2 * QUAD * ff), BF16),
            pltpu.VMEM((QUAD * ff, width), BF16),
            pltpu.VMEM((rows, 2 * QUAD * ff), BF16),
            pltpu.VMEM((rows, QUAD * ff), BF16),
            pltpu.VMEM((width, wide), BF16),
            pltpu.VMEM((rows, width), F32),
            pltpu.VMEM((rows, width), F32),
            pltpu.VMEM((rows, E), F32),
            pltpu.SemaphoreType.DMA((ways,)),
            pltpu.SemaphoreType.DMA((3 * QUAD + 9,)),
        ],
        compiler_params=pltpu.CompilerParams(vmem_limit_bytes=44 << 20),
        cost_estimate=pl.CostEstimate(
            flops=flops, bytes_accessed=moved, transcendentals=QUAD * rows * ff
        ),
    )(own_gate, got_gate, own_x, got_x, dy, w_gate, w_up, w_down, *(carry if carry is not None else ()))


def unpack_kernel(quads, *refs):
    keeps, gots = refs[:quads], refs[quads : 2 * quads]
    gate_ref, up_ref, down_ref = refs[2 * quads :]
    ff = gate_ref.shape[2]
    for quad in range(quads):
        for j in range(QUAD):
            def part(first):
                at = slice(first * ff, (first + 1) * ff)
                return keeps[quad][0, :, at].astype(F32) + gots[quad][0, :, at].astype(F32)

            gate_ref[quad * QUAD + j] = part(2 * j)
            up_ref[quad * QUAD + j] = part(2 * j + 1)
            down_ref[quad * QUAD + j] = part(2 * QUAD + j).T


def unpack(keeps, gots, ff):
    piece = keeps[0].shape[1]
    experts = QUAD * len(keeps)
    vmem = pl.BlockSpec(memory_space=pltpu.VMEM)
    flat = jax.ShapeDtypeStruct((experts, piece, ff), F32)
    return pl.pallas_call(
        functools.partial(unpack_kernel, len(keeps)),
        out_shape=(flat, flat, jax.ShapeDtypeStruct((experts, ff, piece), F32)),
        in_specs=[vmem] * (2 * len(keeps)),
        out_specs=(vmem,) * 3,
        cost_estimate=pl.CostEstimate(
            flops=experts * piece * ff * 3, bytes_accessed=experts * piece * ff * 24, transcendentals=0
        ),
        name="unpack",
    )(*keeps, *gots)


SUB = 256


def rope_packed(rows):
    half_width = HEAD_SIZE // 2
    frequency = (10000.0 ** (-(np.arange(half_width, dtype=np.float32) * 2.0 / HEAD_SIZE))).astype(np.float32)
    angles = np.arange(rows, dtype=np.float32)[:, None] * frequency[None, :]
    pair = np.concatenate([np.cos(angles), np.sin(angles)], axis=1).astype(np.float32)
    return np.concatenate([pair, pair], axis=1)


def lanes_of(array):
    return lax.broadcasted_iota(jnp.int32, array.shape, array.ndim - 1)


def turn(values, table, sign):
    low = lanes_of(values) % HEAD_SIZE < HEAD_SIZE // 2
    down = HEAD_SIZE // 2
    up = 2 * HEAD_SIZE - down
    cosine = jnp.where(low, table, pltpu.roll(table, down, 1))
    sine = jnp.where(low, -pltpu.roll(table, up, 1), table)
    partner = jnp.where(low, pltpu.roll(values, up, 1), pltpu.roll(values, down, 1))
    return values * cosine + sign * (partner * sine)


def seen(start_ref, kind_ref, length, first_row):
    key = lax.broadcasted_iota(jnp.int32, (length, 1), 0)
    row = lax.broadcasted_iota(jnp.int32, (1, SUB), 1) + first_row
    key_piece = jnp.full((length, 1), -1, jnp.int32)
    row_piece = jnp.full((1, SUB), -2, jnp.int32)
    for piece in range(2):
        start = start_ref[0, piece]
        start = jnp.where(kind_ref[0, piece] == 1, start, -2 * PIECE)
        key_piece = jnp.where((key >= start) & (key < start + PIECE), piece, key_piece)
        row_piece = jnp.where((row >= start) & (row < start + PIECE), piece, row_piece)
    return (key <= row) | (key_piece == row_piece)


def attend_kernel(start_ref, kind_ref, tok_ref, gain_ref, wq_ref, wk_ref, wv_ref, table_ref, *refs):
    n1_ref, qm_ref, k2_ref, v2_ref, out_ref, lse_ref, r1_ref, v2t = refs
    rows, _ = tok_ref.shape
    scale = HEAD_SIZE ** (-0.5)

    def project(i, _):
        at = pl.ds(pl.multiple_of(i * SUB, SUB), SUB)
        x = tok_ref[at, :].astype(F32)
        inv = lax.rsqrt(jnp.mean(x * x, axis=1, keepdims=True) + epsilon)
        r1_ref[at, :] = jnp.broadcast_to(inv, (SUB, 128))
        normed = (x * inv * gain_ref[...]).astype(BF16)
        n1_ref[at, :] = normed
        table = table_ref[at, :]
        qp = mm(normed, wq_ref[...], ((1,), (0,)))
        for g in range(2):
            q = turn(qp[:, g * 128 : (g + 1) * 128], table, 1.0)
            left = lanes_of(q) < HEAD_SIZE
            qm_ref[2 * g, at, :] = jnp.where(left, q, 0.0).astype(BF16)
            qm_ref[2 * g + 1, at, :] = jnp.where(left, 0.0, q).astype(BF16)
        k = turn(mm(normed, wk_ref[...], ((1,), (0,))), table, 1.0)
        v = mm(normed, wv_ref[...], ((1,), (0,)))
        left = lanes_of(k) < HEAD_SIZE
        for values, target in ((k, k2_ref), (v, v2_ref)):
            other = pltpu.roll(values, HEAD_SIZE, 1)
            target[0, at, :] = jnp.where(left, values, other).astype(BF16)
            target[1, at, :] = jnp.where(left, other, values).astype(BF16)
        for g in range(2):
            v2t[g, :, at] = v2_ref[g, at, :].T
        return 0

    lax.fori_loop(0, rows // SUB, project, 0)
    lse_ref[...] = jnp.zeros_like(lse_ref)
    for block in range(rows // QBLK):
        length = (block + 1) * QBLK

        def part(i, _):
            first_row = block * QBLK + i * SUB
            at = pl.ds(pl.multiple_of(first_row, SUB), SUB)
            visible = seen(start_ref, kind_ref, length, first_row)
            visible = jnp.concatenate([visible.astype(F32)] * 2, axis=1) > 0.0
            for g in range(2):
                q = jnp.concatenate([qm_ref[2 * g, at, :], qm_ref[2 * g + 1, at, :]], axis=0)
                scores = mm(k2_ref[g, :length, :], q, ((1,), (1,))) * scale
                scores = jnp.where(visible, scores, negative)
                top = jnp.max(scores, axis=0, keepdims=True)
                probs = jnp.exp(scores - top)
                total = jnp.sum(probs, axis=0, keepdims=True)
                probs = (probs * (1.0 / total)).astype(BF16)
                lse = top + jnp.log(total)
                lse_ref[2 * g : 2 * g + 1, at] = lse[:, :SUB]
                lse_ref[2 * g + 1 : 2 * g + 2, at] = lse[:, SUB:]
                res = mm(v2t[g, :, :length], probs, ((1,), (0,)))
                even = lax.broadcasted_iota(jnp.int32, (2 * HEAD_SIZE, SUB), 0) < HEAD_SIZE
                res = jnp.where(even, res[:, :SUB], res[:, SUB:])
                out_ref[at, g * 128 : (g + 1) * 128] = res.T.astype(BF16)
            return 0

        lax.fori_loop(0, QBLK // SUB, part, 0)


def attend(piece_start, piece_kind, tokens, gain, wq, wk, wv, table):
    rows, width = tokens.shape
    vmem = pl.BlockSpec(memory_space=pltpu.VMEM)
    smem = pl.BlockSpec(memory_space=pltpu.SMEM)

    def shape(*dims, dtype=BF16):
        return jax.ShapeDtypeStruct(dims, dtype)

    return pl.pallas_call(
        attend_kernel,
        out_shape=(
            shape(rows, width),
            shape(4, rows, 128),
            shape(2, rows, 128),
            shape(2, rows, 128),
            shape(rows, 256),
            shape(8, rows, dtype=F32),
            shape(rows, 128, dtype=F32),
        ),
        in_specs=[smem, smem] + [vmem] * 6,
        out_specs=(vmem,) * 7,
        scratch_shapes=[pltpu.VMEM((2, 128, rows), BF16)],
        compiler_params=pltpu.CompilerParams(vmem_limit_bytes=40 << 20),
        cost_estimate=pl.CostEstimate(
            flops=6 << 30, bytes_accessed=8 << 20, transcendentals=4 * rows * rows
        ),
        name="attend",
    )(piece_start, piece_kind, tokens, gain[None, :], wq, wk, wv, table)


def place_blocks(source, keep, send, ways, order, sems):
    me = lax.axis_index("dp")
    piece = source.shape[0] // ways
    half = ways // 2
    copies = []
    for slot in range(ways):
        dest = 0
        for place, bit in enumerate(order):
            own = (slot >> (len(order) - 1 - place)) & 1
            dest = dest + ((me // (1 << bit) + own) % 2) * (1 << bit)
        block = source.at[pl.ds(pl.multiple_of(dest * piece, piece), piece), :]
        target = keep.at[slot] if slot < half else send.at[slot - half]
        copies.append(pltpu.make_async_copy(block, target, sems.at[slot]))
    return copies


def attend_back_kernel(ways, order, start_ref, kind_ref, qm_ref, k2_ref, v2_ref, lse_ref, o_ref, n1_ref, tok_ref, *refs):
    r1_ref, wq_ref, wk_ref, wv_ref, wo_ref, table_ref, own_do, got_do = refs[:8]
    keep, send, dn_own, dn_other, gain_ref = refs[8:13]
    do, dom, do_t, n1_t, k2t, dk_acc, dv_acc, gqkv, wqkv, grads, dn, block_sem, sem = refs[13:]
    rows, width = tok_ref.shape
    scale = HEAD_SIZE ** (-0.5)
    core = lax.axis_index("tensor") % 2
    half = rows // 2
    own_at = pl.ds(pl.multiple_of(core * half, half), half)
    other_at = pl.ds(pl.multiple_of((1 - core) * half, half), half)
    loads = (
        pltpu.make_async_copy(own_do, do.at[own_at, :], sem.at[0]),
        pltpu.make_async_copy(got_do, do.at[other_at, :], sem.at[1]),
    )
    for load in loads:
        load.start()
    wqkv[:, :256] = wq_ref[...]
    wqkv[:, 256:384] = wk_ref[...]
    wqkv[:, 384:] = wv_ref[...]
    dk_acc[...] = jnp.zeros_like(dk_acc)
    dv_acc[...] = jnp.zeros_like(dv_acc)
    for load in loads:
        load.wait()

    def prepare(i, _):
        at = pl.ds(pl.multiple_of(i * SUB, SUB), SUB)
        block = do[at, :]
        dob = mm(block, wo_ref[...], ((1,), (1,)))
        for g in range(2):
            pair = dob[:, g * 128 : (g + 1) * 128]
            left = lanes_of(pair) < HEAD_SIZE
            dom[2 * g, at, :] = jnp.where(left, pair, 0.0).astype(BF16)
            dom[2 * g + 1, at, :] = jnp.where(left, 0.0, pair).astype(BF16)
            k2t[g, :, at] = k2_ref[g, at, :].T
        do_t[:, at] = block.T
        n1_t[:, at] = n1_ref[at, :].T
        return 0

    lax.fori_loop(0, rows // SUB, prepare, 0)
    for block in range(rows // QBLK):
        length = (block + 1) * QBLK

        def part(i, _):
            first_row = block * QBLK + i * SUB
            at = pl.ds(pl.multiple_of(first_row, SUB), SUB)
            visible = seen(start_ref, kind_ref, length, first_row)
            visible = jnp.concatenate([visible.astype(F32)] * 2, axis=1) > 0.0
            table = table_ref[at, :]
            for g in range(2):
                q = jnp.concatenate([qm_ref[2 * g, at, :], qm_ref[2 * g + 1, at, :]], axis=0)
                dob = jnp.concatenate([dom[2 * g, at, :], dom[2 * g + 1, at, :]], axis=0)
                lse = jnp.concatenate([lse_ref[2 * g : 2 * g + 1, at], lse_ref[2 * g + 1 : 2 * g + 2, at]], axis=1)
                scores = mm(k2_ref[g, :length, :], q, ((1,), (1,))) * scale
                probs = jnp.exp(jnp.where(visible, scores, negative) - lse)
                dp = mm(v2_ref[g, :length, :], dob, ((1,), (1,)))
                delta = jnp.sum(probs * dp, axis=0, keepdims=True)
                ds = (probs * (dp - delta)).astype(BF16)
                dk_acc[g, :length, :] += mm(ds, q, ((1,), (0,)))
                dv_acc[g, :length, :] += mm(probs.astype(BF16), dob, ((1,), (0,)))
                dq = mm(k2t[g, :, :length], ds, ((1,), (0,)))
                even = lax.broadcasted_iota(jnp.int32, (2 * HEAD_SIZE, SUB), 0) < HEAD_SIZE
                dq = jnp.where(even, dq[:, :SUB], dq[:, SUB:]).T * scale
                gqkv[at, g * 128 : (g + 1) * 128] = turn(dq, table, -1.0).astype(BF16)
            return 0

        lax.fori_loop(0, QBLK // SUB, part, 0)

    def close(i, _):
        at = pl.ds(pl.multiple_of(i * SUB, SUB), SUB)

        def folded(acc):
            first, second = acc[0, at, :], acc[1, at, :]
            left = lanes_of(first) < HEAD_SIZE
            first = first + pltpu.roll(first, HEAD_SIZE, 1)
            second = second + pltpu.roll(second, HEAD_SIZE, 1)
            return jnp.where(left, first, second)

        gqkv[at, 256:384] = turn(folded(dk_acc) * scale, table_ref[at, :], -1.0).astype(BF16)
        gqkv[at, 384:] = folded(dv_acc).astype(BF16)
        return 0

    lax.fori_loop(0, rows // SUB, close, 0)

    def weight_rows(i, _):
        at = pl.ds(pl.multiple_of(i * SUB, SUB), SUB)
        grads[at, :512] = mm(n1_t[at, :], gqkv[...], ((1,), (0,))).astype(BF16)
        grads[at, 512:] = mm(do_t[at, :], o_ref[...], ((1,), (0,))).astype(BF16)
        return 0

    lax.fori_loop(0, width // SUB, weight_rows, 0)
    copies = place_blocks(grads, keep, send, ways, order, block_sem)
    for copy in copies:
        copy.start()
    gain_ref[...] = jnp.zeros_like(gain_ref)

    def data_rows(i, _):
        at = pl.ds(pl.multiple_of(i * SUB, SUB), SUB)
        grad = mm(gqkv[at, :], wqkv[...], ((1,), (1,)))
        dn[at, :] = grad.astype(BF16)
        by = grad * (tok_ref[at, :].astype(F32) * r1_ref[at, :1])
        gain_ref[0:1, :] += jnp.sum(by, axis=0, keepdims=True)
        return 0

    lax.fori_loop(0, rows // SUB, data_rows, 0)
    saves = (
        pltpu.make_async_copy(dn.at[own_at, :], dn_own, sem.at[0]),
        pltpu.make_async_copy(dn.at[other_at, :], dn_other, sem.at[1]),
    )
    for copy in saves:
        copy.start()
    for copy in copies:
        copy.wait()
    for copy in saves:
        copy.wait()


def attend_back(ways, order, piece_start, piece_kind, saved, tokens, weights, table, own_do, got_do):
    n1, qm, k2, v2, out, lse, r1 = saved
    wq, wk, wv, wo = weights
    rows, width = tokens.shape
    vmem = pl.BlockSpec(memory_space=pltpu.VMEM)
    smem = pl.BlockSpec(memory_space=pltpu.SMEM)
    any_space = pl.BlockSpec(memory_space=pl.ANY)
    block = jax.ShapeDtypeStruct((ways // 2, width // ways, 768), BF16)
    half = jax.ShapeDtypeStruct((rows // 2, width), BF16)
    return pl.pallas_call(
        functools.partial(attend_back_kernel, ways, order),
        out_shape=(block, block, half, half, jax.ShapeDtypeStruct((8, width), F32)),
        in_specs=[smem, smem] + [vmem] * 13 + [any_space] * 2,
        out_specs=(any_space,) * 4 + (vmem,),
        scratch_shapes=[
            pltpu.VMEM((rows, width), BF16),
            pltpu.VMEM((4, rows, 128), BF16),
            pltpu.VMEM((width, rows), BF16),
            pltpu.VMEM((width, rows), BF16),
            pltpu.VMEM((2, 128, rows), BF16),
            pltpu.VMEM((2, rows, 128), F32),
            pltpu.VMEM((2, rows, 128), F32),
            pltpu.VMEM((rows, 512), BF16),
            pltpu.VMEM((width, 512), BF16),
            pltpu.VMEM((width, 768), BF16),
            pltpu.VMEM((rows, width), BF16),
            pltpu.SemaphoreType.DMA((ways,)),
            pltpu.SemaphoreType.DMA((2,)),
        ],
        compiler_params=pltpu.CompilerParams(vmem_limit_bytes=44 << 20),
        cost_estimate=pl.CostEstimate(
            flops=12 << 30, bytes_accessed=16 << 20, transcendentals=4 * rows * rows
        ),
        name="attend_back",
    )(piece_start, piece_kind, qm, k2, v2, lse, out, n1, tokens, r1, wq, wk, wv, wo, table, own_do, got_do)


def make_body(ways):
    def body(
        tokens,
        w_query,
        key_weight,
        value_weight,
        w_output,
        gain_attn,
        gain_ffn,
        router,
        w_gate,
        w_up,
        w_down,
        piece_start,
        piece_kind,
        choices,
        place_order,
        cotangent,
    ):
        rows = tokens.shape[0]
        half = rows // 2
        width = tokens.shape[1]
        core = lax.axis_index("tensor") % 2

        def my_half(array):
            return lax.dynamic_slice_in_dim(array, core * half, half, 0)

        from_x = lax.ppermute(w_output, "tensor", X_PAIRS)
        near = jnp.stack([w_output, from_x])
        far = lax.ppermute(near, "tensor", CORE_PAIRS)
        all_output = jnp.concatenate([w_output, far[0], from_x, far[1]], axis=0)
        resid_in = tokens.astype(F32)
        table = jnp.asarray(rope_packed(rows))
        saved = attend(
            piece_start, piece_kind, tokens, gain_attn, w_query, key_weight, value_weight, table
        )
        head_out = saved[4]
        mine = my_half(head_out)
        other = lax.dynamic_slice_in_dim(head_out, (1 - core) * half, half, 0)
        chip_heads = jnp.concatenate([mine, lax.ppermute(other, "tensor", CORE_PAIRS)], axis=1)
        far_heads = lax.ppermute(chip_heads, "tensor", X_PAIRS)
        all_heads = jnp.concatenate([chip_heads, far_heads], axis=1)
        mid = my_half(resid_in) + mm(all_heads, all_output, ((1,), (0,)))
        inv_two = lax.rsqrt(jnp.mean(mid * mid, axis=1, keepdims=True) + epsilon)
        normed_half = (mid * inv_two * gain_ffn).astype(BF16)
        normed_far = lax.ppermute(normed_half, "tensor", CORE_PAIRS)

        expert_ids = jnp.arange(E, dtype=jnp.int32)
        picked = jnp.any(choices[:, :, None] == expert_ids[None, None, :], axis=1)
        ranks = place_order[0]
        earlier = (ranks[None, :] < ranks[:, None]).astype(BF16)
        slot = mm(earlier, picked.astype(BF16), ((1,), (0,)))
        kept = (picked & (slot < CAP)).astype(F32)
        picked_half = my_half(picked.astype(F32))
        kept_half = my_half(kept)
        logits = mm(normed_half, router, ((1,), (0,)))
        logits = jnp.where(picked_half > 0, logits, negative)
        gates_half = jax.nn.softmax(logits, axis=1)
        gates_half = jnp.where(picked_half > 0, gates_half, 0.0)
        slot_gate = gates_half * kept_half
        slot_gate_far = lax.ppermute(slot_gate, "tensor", CORE_PAIRS)

        piece = width // ways
        ff = w_gate.shape[2]
        plain = bits_of(ways)
        turned = plain[1:] + plain[:1]
        shared = (slot_gate, slot_gate_far, normed_half, normed_far, cotangent, w_gate, w_up, w_down)
        orders = (plain, turned, plain, plain)
        carry = None
        dg_parts, keeps, gots = [], [], []
        for quad in range(E // QUAD):
            result = run_experts(quad, orders[quad], ways, *shared, carry)
            dg_part, norm_part, moe_part, keep, send = result[:5]
            carry = (result[5:] if quad == 0 else carry[:2]) + (norm_part, moe_part)
            dg_parts.append(dg_part[:, quad * QUAD : (quad + 1) * QUAD])
            keep, got = halve(keep, send, ways, orders[quad])
            keeps.append(keep)
            gots.append(got)
        sent_gate, sent_up, sent_down = unpack(keeps, gots, ff)
        grad_gate_part = jnp.concatenate(dg_parts, axis=1) * kept

        norm_near, norm_far = reduce_half(norm_part, core)
        norm_half = norm_near.astype(F32) + norm_far.astype(F32)
        dg_near, dg_far = reduce_half(grad_gate_part, core)
        dg_half = dg_near.astype(F32) + dg_far.astype(F32)
        moe_near, moe_far = reduce_half(moe_part, core)
        dz = gates_half * (dg_half - jnp.sum(gates_half * dg_half, axis=1, keepdims=True))
        dlg = dz.astype(BF16)
        grad_norm = norm_half + mm(dlg, router, ((1,), (1,)))
        grad_router = mm(dlg, normed_half, ((0,), (0,)))
        grad_gain_ffn = jnp.sum(grad_norm * mid * inv_two, axis=0)
        scaled = gain_ffn * grad_norm
        grad_mid = (
            my_half(cotangent).astype(F32)
            + inv_two * scaled
            - mid * inv_two**3 * jnp.mean(scaled * mid, axis=1, keepdims=True)
        )
        own_do = grad_mid.astype(BF16)
        got_do = lax.ppermute(own_do, "tensor", CORE_PAIRS)
        keep, send, dn_own, dn_other, gain_rows = attend_back(
            ways,
            plain,
            piece_start,
            piece_kind,
            saved,
            tokens,
            (w_query, key_weight, value_weight, w_output),
            table,
            own_do,
            got_do,
        )
        grad_gain_attn = gain_rows[0]
        moe_far, dn_own = lax.optimization_barrier((moe_far, dn_own))
        output = (mid + (moe_near.astype(F32) + moe_far.astype(F32))).astype(BF16)
        output = share_half(output, core)
        keep, got = halve(keep, send, ways, plain)
        sent_attn = keep[0].astype(F32) + got[0].astype(F32)
        nq, nk = w_query.shape[1], key_weight.shape[1]
        dn_got = lax.ppermute(dn_other, "tensor", CORE_PAIRS)
        last_near = (dn_own.astype(F32) + dn_got.astype(F32)).astype(BF16)
        last_far = lax.ppermute(last_near, "tensor", X_PAIRS)
        norm_one_half = last_near.astype(F32) + last_far.astype(F32)
        x_half = my_half(resid_in)
        inv_half = lax.rsqrt(jnp.mean(x_half * x_half, axis=1, keepdims=True) + epsilon)
        scaled_one = gain_attn * norm_one_half
        input_half = (
            grad_mid
            + inv_half * scaled_one
            - x_half * inv_half**3 * jnp.mean(scaled_one * x_half, axis=1, keepdims=True)
        ).astype(BF16)
        input_grad = share_half(input_half, core)
        first_chip = (lax.axis_index("tensor") < 2).astype(F32)
        row_sums = jnp.concatenate([grad_gain_ffn[None], grad_router], axis=0) * first_chip
        small = jnp.concatenate([grad_gain_attn[None], row_sums], axis=0)
        small = small + lax.ppermute(small, "tensor", CORE_PAIRS)
        small = small + lax.ppermute(small, "tensor", X_PAIRS)
        count = small.shape[0]
        small = small.reshape(count, ways, piece).transpose(1, 0, 2)
        (small,) = scatter_sums((small,), ways, plain)
        return (
            output,
            input_grad,
            sent_attn[:, :nq],
            sent_attn[:, nq : nq + nk],
            sent_attn[:, nq + nk : nq + 2 * nk],
            sent_attn[:, nq + 2 * nk :].T,
            small[0],
            small[1],
            small[2:].T,
            sent_gate,
            sent_up,
            sent_down,
        )

    return body


def solution(mesh):
    body = make_body(mesh.shape["dp"])

    return jax.shard_map(
        body,
        mesh=mesh,
        in_specs=(
            P("dp", None),
            P(None, "tensor"),
            P(None, "tensor"),
            P(None, "tensor"),
            P("tensor", None),
            P(),
            P(),
            P(),
            P(None, None, "tensor"),
            P(None, None, "tensor"),
            P(None, "tensor", None),
            P("dp", None),
            P("dp", None),
            P("dp", None),
            P("dp", None),
            P("dp", None),
        ),
        out_specs=(
            P("dp", None),
            P("dp", None),
            P("dp", "tensor"),
            P("dp", "tensor"),
            P("dp", "tensor"),
            P("tensor", "dp"),
            P("dp"),
            P("dp"),
            P("dp", None),
            P(None, "dp", "tensor"),
            P(None, "dp", "tensor"),
            P(None, "tensor", "dp"),
        ),
        check_vma=False,
    )
```

```python
import functools

import jax
import jax.numpy as jnp
import numpy as np
from jax import lax
from jax.experimental import pallas as pl
from jax.experimental.pallas import tpu as pltpu
from jax.sharding import PartitionSpec as P


HEAD_SIZE = 64
E = 16
PIECE = 256
QBLK = 512
CAP = 640

epsilon = 1e-06
negative = -1e30
F32 = jnp.float32
BF16 = jnp.bfloat16


def mm(left, right, dims):
    return lax.dot_general(left, right, (dims, ((), ())), preferred_element_type=F32)


CORE_PAIRS = [(i, i ^ 1) for i in range(4)]
X_PAIRS = [(i, i ^ 2) for i in range(4)]


def reduce_pair(mine, other):
    got = lax.ppermute(other, "tensor", CORE_PAIRS)
    total = (mine.astype(F32) + got.astype(F32)).astype(BF16)
    far = lax.ppermute(total, "tensor", X_PAIRS)
    return total, far


def share_half(half_rows, core):
    got = lax.ppermute(half_rows, "tensor", CORE_PAIRS)
    pair = jnp.stack([jnp.where(core == 0, half_rows, got), jnp.where(core == 0, got, half_rows)])
    return pair.reshape((2 * half_rows.shape[0],) + half_rows.shape[1:])


def bits_of(ways):
    return tuple(range(ways.bit_length() - 1))


def flip(array, ways, bit):
    return lax.ppermute(array, "dp", [(i, i ^ (1 << bit)) for i in range(ways)])


def halve(keep, send, ways, order):
    got = flip(send, ways, order[0])
    for bit in order[1:]:
        half = keep.shape[0] // 2
        to_send = (keep[half:].astype(F32) + got[half:].astype(F32)).astype(keep.dtype)
        keep = (keep[:half].astype(F32) + got[:half].astype(F32)).astype(keep.dtype)
        got = flip(to_send, ways, bit)
    return keep, got


def scatter_sums(arrays, ways, order):
    me = lax.axis_index("dp")
    count = len(order)
    current = [blocks.reshape((2,) * count + blocks.shape[1:]) for blocks in arrays]
    left = list(reversed(range(count)))
    for bit in order:
        axis = left.index(bit)
        mine_at = (me >> bit) & 1
        left.remove(bit)
        for i, blocks in enumerate(current):
            mine = lax.dynamic_index_in_dim(blocks, mine_at, axis, keepdims=False)
            other = lax.dynamic_index_in_dim(blocks, 1 - mine_at, axis, keepdims=False)
            got = flip(other, ways, bit)
            total = mine.astype(F32) + got.astype(F32)
            current[i] = total.astype(blocks.dtype) if left else total
    return current


QUAD = 4
ROWS = 512


def expert_kernel(first, ways, order, carried, last, *refs):
    own_gate, got_gate, own_x, got_x, dy_hbm, wg_hbm, wu_hbm, wd_hbm = refs[:8]
    refs = refs[8:]
    if carried:
        xt_hbm, dyt_hbm, norm_in, moe_in, dg_ref = refs[:5]
        count = 4 if last else 2
        sums, keep, send = refs[5 : 5 + count], refs[5 + count], refs[6 + count]
        refs = refs[7 + count :]
    else:
        dg_ref, *sums, keep, send, xt_hbm, dyt_hbm = refs[:7]
        refs = refs[7:]
    x_ref, xt_ref, dy_ref, dyt_ref, wgu, wd, gu, gated, grads, norm_acc, moe_acc = refs[:11]
    gate_ref, *rounded, block_sem, sem = refs[11:]
    rows, width = x_ref.shape
    ff = wg_hbm.shape[2]

    loads = []
    for j in range(QUAD):
        gate_at = pl.ds(2 * j * ff, ff)
        up_at = pl.ds((2 * j + 1) * ff, ff)
        loads.append(pltpu.make_async_copy(wg_hbm.at[first + j], wgu.at[:, gate_at], sem.at[j]))
        loads.append(pltpu.make_async_copy(wu_hbm.at[first + j], wgu.at[:, up_at], sem.at[QUAD + j]))
    for j in range(QUAD):
        down_at = pl.ds(j * ff, ff)
        loads.append(pltpu.make_async_copy(wd_hbm.at[first + j], wd.at[down_at, :], sem.at[2 * QUAD + j]))
    core = lax.axis_index("tensor") % 2
    rows_half = rows // 2
    own_at = pl.ds(pl.multiple_of(core * rows_half, rows_half), rows_half)
    got_at = pl.ds(pl.multiple_of((1 - core) * rows_half, rows_half), rows_half)
    loads = [
        pltpu.make_async_copy(own_x, x_ref.at[own_at, :], sem.at[3 * QUAD]),
        pltpu.make_async_copy(got_x, x_ref.at[got_at, :], sem.at[3 * QUAD + 6]),
    ] + loads
    loads.append(pltpu.make_async_copy(own_gate, gate_ref.at[own_at, :], sem.at[3 * QUAD + 7]))
    loads.append(pltpu.make_async_copy(got_gate, gate_ref.at[got_at, :], sem.at[3 * QUAD + 8]))
    loads.append(pltpu.make_async_copy(dy_hbm, dy_ref, sem.at[3 * QUAD + 1]))
    for load in loads:
        load.start()
    if carried:
        load_norm = pltpu.make_async_copy(norm_in, norm_acc, sem.at[3 * QUAD + 4])
        load_moe = pltpu.make_async_copy(moe_in, moe_acc, sem.at[3 * QUAD + 5])
        load_xt = pltpu.make_async_copy(xt_hbm, xt_ref, sem.at[3 * QUAD + 2])
        load_dyt = pltpu.make_async_copy(dyt_hbm, dyt_ref, sem.at[3 * QUAD + 3])
        for load in (load_norm, load_moe, load_xt, load_dyt):
            load.start()
    dg_ref[...] = jnp.zeros_like(dg_ref)
    for load in loads:
        load.wait()
    lane = lax.broadcasted_iota(jnp.int32, (ROWS, dg_ref.shape[1]), 1)

    def hidden_rows(i, _):
        at = pl.ds(pl.multiple_of(i * ROWS, ROWS), ROWS)
        au = mm(x_ref[at, :], wgu[...], ((1,), (0,)))
        down = mm(dy_ref[at, :], wd[...], ((1,), (1,)))
        gate_rows = gate_ref[at, :]
        dg = dg_ref[at, :]
        for j in range(QUAD):
            pre = au[:, 2 * j * ff : (2 * j + 1) * ff]
            up = au[:, (2 * j + 1) * ff : (2 * j + 2) * ff]
            back = down[:, j * ff : (j + 1) * ff]
            gate = gate_rows[:, first + j : first + j + 1]
            sigmoid = 1.0 / (1.0 + jnp.exp(-pre))
            act = pre * sigmoid
            hidden = act * up
            gated[at, j * ff : (j + 1) * ff] = (gate * hidden).astype(BF16)
            row = jnp.sum(hidden * back, axis=1, keepdims=True)
            dg = jnp.where(lane == first + j, row, dg)
            back = gate * back
            slope = sigmoid * (1.0 + pre * (1.0 - sigmoid))
            gu[at, 2 * j * ff : (2 * j + 1) * ff] = (back * up * slope).astype(BF16)
            gu[at, (2 * j + 1) * ff : (2 * j + 2) * ff] = (back * act).astype(BF16)
        dg_ref[at, :] = dg
        return 0

    lax.fori_loop(0, rows // ROWS, hidden_rows, 0)
    if carried:
        load_norm.wait()
        load_moe.wait()

    def data_rows(i, _):
        at = pl.ds(pl.multiple_of(i * ROWS, ROWS), ROWS)
        norm = mm(gu[at, :], wgu[...], ((1,), (1,)))
        moe = mm(gated[at, :], wd[...], ((1,), (0,)))
        if last:
            rounded[0][at, :] = (norm_acc[at, :] + norm).astype(BF16)
            rounded[1][at, :] = (moe_acc[at, :] + moe).astype(BF16)
        elif carried:
            norm_acc[at, :] += norm
            moe_acc[at, :] += moe
        else:
            norm_acc[at, :] = norm
            moe_acc[at, :] = moe
            xt_ref[:, at] = x_ref[at, :].T
            dyt_ref[:, at] = dy_ref[at, :].T
        return 0

    lax.fori_loop(0, rows // ROWS, data_rows, 0)
    if last:
        parts = [total.at[at, :] for total in rounded for at in (own_at, got_at)]
    else:
        parts = [norm_acc, moe_acc]
    saves = [
        pltpu.make_async_copy(part, target, sem.at[3 * QUAD + 4 + i])
        for i, (part, target) in enumerate(zip(parts, sums))
    ]
    for save in saves:
        save.start()
    if carried:
        load_xt.wait()
        load_dyt.wait()
    else:
        save_xt = pltpu.make_async_copy(xt_ref, xt_hbm, sem.at[3 * QUAD + 2])
        save_dyt = pltpu.make_async_copy(dyt_ref, dyt_hbm, sem.at[3 * QUAD + 3])
        save_xt.start()
        save_dyt.start()

    def grad_rows(i, _):
        at = pl.ds(pl.multiple_of(i * ROWS, ROWS), ROWS)
        grads[at, : 2 * QUAD * ff] = mm(xt_ref[at, :], gu[...], ((1,), (0,))).astype(BF16)
        grads[at, 2 * QUAD * ff :] = mm(dyt_ref[at, :], gated[...], ((1,), (0,))).astype(BF16)
        return 0

    lax.fori_loop(0, width // ROWS, grad_rows, 0)
    copies = place_blocks(grads, keep, send, ways, order, block_sem)
    for copy in copies:
        copy.start()
    for copy in copies:
        copy.wait()
    for save in saves:
        save.wait()
    if not carried:
        save_xt.wait()
        save_dyt.wait()


def run_experts(quad, order, ways, own_gate, got_gate, own_x, got_x, dy, w_gate, w_up, w_down, carry):
    rows, width = dy.shape
    ff = w_gate.shape[2]
    piece = width // ways
    any_space = pl.BlockSpec(memory_space=pl.ANY)
    vmem = pl.BlockSpec(memory_space=pltpu.VMEM)
    wide = 3 * QUAD * ff
    block = jax.ShapeDtypeStruct((ways // 2, piece, wide), BF16)
    last = quad == E // QUAD - 1
    if last:
        totals = (jax.ShapeDtypeStruct((rows // 2, width), BF16),) * 4
    else:
        totals = (jax.ShapeDtypeStruct((rows, width), F32),) * 2
    turned = jax.ShapeDtypeStruct((width, rows), BF16)
    flops = 2 * 9 * QUAD * rows * width * ff
    moved = QUAD * width * ff * 12 + rows * width * 8 + rows * width * 16
    return pl.pallas_call(
        functools.partial(expert_kernel, quad * QUAD, ways, order, carry is not None, last),
        out_shape=(jax.ShapeDtypeStruct((rows, 128), F32),)
        + totals
        + (block, block)
        + ((turned, turned) if carry is None else ()),
        in_specs=[any_space] * (8 if carry is None else 12),
        out_specs=(vmem,) + (any_space,) * (len(totals) + (4 if carry is None else 2)),
        scratch_shapes=[
            pltpu.VMEM((rows, width), BF16),
            pltpu.VMEM((width, rows), BF16),
            pltpu.VMEM((rows, width), BF16),
            pltpu.VMEM((width, rows), BF16),
            pltpu.VMEM((width, 2 * QUAD * ff), BF16),
            pltpu.VMEM((QUAD * ff, width), BF16),
            pltpu.VMEM((rows, 2 * QUAD * ff), BF16),
            pltpu.VMEM((rows, QUAD * ff), BF16),
            pltpu.VMEM((width, wide), BF16),
            pltpu.VMEM((rows, width), F32),
            pltpu.VMEM((rows, width), F32),
            pltpu.VMEM((rows, E), F32),
        ]
        + [pltpu.VMEM((rows, width), BF16)] * (2 if last else 0)
        + [
            pltpu.SemaphoreType.DMA((ways,)),
            pltpu.SemaphoreType.DMA((3 * QUAD + 9,)),
        ],
        compiler_params=pltpu.CompilerParams(vmem_limit_bytes=VMEM_BYTES),
        cost_estimate=pl.CostEstimate(
            flops=flops, bytes_accessed=moved, transcendentals=QUAD * rows * ff
        ),
    )(own_gate, got_gate, own_x, got_x, dy, w_gate, w_up, w_down, *(carry if carry is not None else ()))


def unpack_kernel(quads, *refs):
    keeps, gots = refs[:quads], refs[quads : 2 * quads]
    gate_ref, up_ref, down_ref = refs[2 * quads :]
    ff = gate_ref.shape[2]
    for quad in range(quads):
        for j in range(QUAD):
            def part(first):
                at = slice(first * ff, (first + 1) * ff)
                return keeps[quad][0, :, at].astype(F32) + gots[quad][0, :, at].astype(F32)

            gate_ref[quad * QUAD + j] = part(2 * j)
            up_ref[quad * QUAD + j] = part(2 * j + 1)
            down_ref[quad * QUAD + j] = part(2 * QUAD + j).T


def unpack(keeps, gots, ff):
    piece = keeps[0].shape[1]
    experts = QUAD * len(keeps)
    vmem = pl.BlockSpec(memory_space=pltpu.VMEM)
    flat = jax.ShapeDtypeStruct((experts, piece, ff), F32)
    return pl.pallas_call(
        functools.partial(unpack_kernel, len(keeps)),
        out_shape=(flat, flat, jax.ShapeDtypeStruct((experts, ff, piece), F32)),
        in_specs=[vmem] * (2 * len(keeps)),
        out_specs=(vmem,) * 3,
        cost_estimate=pl.CostEstimate(
            flops=experts * piece * ff * 3, bytes_accessed=experts * piece * ff * 24, transcendentals=0
        ),
        name="unpack",
    )(*keeps, *gots)


SUB = 256
VMEM_BYTES = 60 << 20


def rope_packed(rows):
    half_width = HEAD_SIZE // 2
    frequency = (10000.0 ** (-(np.arange(half_width, dtype=np.float32) * 2.0 / HEAD_SIZE))).astype(np.float32)
    angles = np.arange(rows, dtype=np.float32)[:, None] * frequency[None, :]
    pair = np.concatenate([np.cos(angles), np.sin(angles)], axis=1).astype(np.float32)
    return np.concatenate([pair, pair], axis=1)


def lanes_of(array):
    return lax.broadcasted_iota(jnp.int32, array.shape, array.ndim - 1)


def turn(values, table, sign):
    low = lanes_of(values) % HEAD_SIZE < HEAD_SIZE // 2
    down = HEAD_SIZE // 2
    up = 2 * HEAD_SIZE - down
    cosine = jnp.where(low, table, pltpu.roll(table, down, 1))
    sine = jnp.where(low, -pltpu.roll(table, up, 1), table)
    partner = jnp.where(low, pltpu.roll(values, up, 1), pltpu.roll(values, down, 1))
    return values * cosine + sign * (partner * sine)


def seen(start_ref, kind_ref, length, first_row):
    key = lax.broadcasted_iota(jnp.int32, (length, 1), 0)
    row = lax.broadcasted_iota(jnp.int32, (1, SUB), 1) + first_row
    key_piece = jnp.full((length, 1), -1, jnp.int32)
    row_piece = jnp.full((1, SUB), -2, jnp.int32)
    for piece in range(2):
        start = start_ref[0, piece]
        start = jnp.where(kind_ref[0, piece] == 1, start, -2 * PIECE)
        key_piece = jnp.where((key >= start) & (key < start + PIECE), piece, key_piece)
        row_piece = jnp.where((row >= start) & (row < start + PIECE), piece, row_piece)
    return (key <= row) | (key_piece == row_piece)


def attend_kernel(start_ref, kind_ref, gain_ref, *refs):
    sources, refs = refs[:5], refs[5:]
    lse_ref, refs = refs[0], refs[1:]
    targets, refs = refs[:8], refs[8:]
    tok_ref, wq_ref, wk_ref, wv_ref, table_ref, n1_ref, qm_ref, k2_ref, v2_ref, r1_ref, out_ref, v2t, sem = refs
    rows, _ = tok_ref.shape
    scale = HEAD_SIZE ** (-0.5)
    loads = [
        pltpu.make_async_copy(source, target, sem.at[i])
        for i, (source, target) in enumerate(zip(sources, (tok_ref, wq_ref, wk_ref, wv_ref, table_ref)))
    ]
    for load in loads:
        load.start()
    for load in loads:
        load.wait()

    def project(i, _):
        at = pl.ds(pl.multiple_of(i * SUB, SUB), SUB)
        x = tok_ref[at, :].astype(F32)
        inv = lax.rsqrt(jnp.mean(x * x, axis=1, keepdims=True) + epsilon)
        r1_ref[at, :] = jnp.broadcast_to(inv, (SUB, 128))
        normed = (x * inv * gain_ref[...]).astype(BF16)
        n1_ref[at, :] = normed
        table = table_ref[at, :]
        qp = mm(normed, wq_ref[...], ((1,), (0,)))
        for g in range(2):
            q = turn(qp[:, g * 128 : (g + 1) * 128], table, 1.0)
            left = lanes_of(q) < HEAD_SIZE
            qm_ref[2 * g, at, :] = jnp.where(left, q, 0.0).astype(BF16)
            qm_ref[2 * g + 1, at, :] = jnp.where(left, 0.0, q).astype(BF16)
        k = turn(mm(normed, wk_ref[...], ((1,), (0,))), table, 1.0)
        v = mm(normed, wv_ref[...], ((1,), (0,)))
        left = lanes_of(k) < HEAD_SIZE
        for values, target in ((k, k2_ref), (v, v2_ref)):
            other = pltpu.roll(values, HEAD_SIZE, 1)
            target[0, at, :] = jnp.where(left, values, other).astype(BF16)
            target[1, at, :] = jnp.where(left, other, values).astype(BF16)
        for g in range(2):
            v2t[g, :, at] = v2_ref[g, at, :].T
        return 0

    lax.fori_loop(0, rows // SUB, project, 0)
    saves = [
        pltpu.make_async_copy(source, target, sem.at[5 + i])
        for i, (source, target) in enumerate(zip((n1_ref, qm_ref, k2_ref, v2_ref, r1_ref), targets))
    ]
    for save in saves:
        save.start()
    lse_ref[...] = jnp.zeros_like(lse_ref)
    for block in range(rows // QBLK):
        length = (block + 1) * QBLK

        def part(i, _):
            first_row = block * QBLK + i * SUB
            at = pl.ds(pl.multiple_of(first_row, SUB), SUB)
            visible = seen(start_ref, kind_ref, length, first_row)
            visible = jnp.concatenate([visible.astype(F32)] * 2, axis=1) > 0.0
            for g in range(2):
                q = jnp.concatenate([qm_ref[2 * g, at, :], qm_ref[2 * g + 1, at, :]], axis=0)
                scores = mm(k2_ref[g, :length, :], q, ((1,), (1,))) * scale
                scores = jnp.where(visible, scores, negative)
                top = jnp.max(scores, axis=0, keepdims=True)
                probs = jnp.exp(scores - top)
                total = jnp.sum(probs, axis=0, keepdims=True)
                probs = (probs * (1.0 / total)).astype(BF16)
                lse = top + jnp.log(total)
                lse_ref[2 * g : 2 * g + 1, at] = lse[:, :SUB]
                lse_ref[2 * g + 1 : 2 * g + 2, at] = lse[:, SUB:]
                res = mm(v2t[g, :, :length], probs, ((1,), (0,)))
                even = lax.broadcasted_iota(jnp.int32, (2 * HEAD_SIZE, SUB), 0) < HEAD_SIZE
                res = jnp.where(even, res[:, :SUB], res[:, SUB:])
                out_ref[at, g * 128 : (g + 1) * 128] = res.T.astype(BF16)
            return 0

        lax.fori_loop(0, QBLK // SUB, part, 0)
    core = lax.axis_index("tensor") % 2
    half = rows // 2
    own_at = pl.ds(pl.multiple_of(core * half, half), half)
    other_at = pl.ds(pl.multiple_of((1 - core) * half, half), half)
    last = [
        pltpu.make_async_copy(out_ref.at[own_at, :], targets[5], sem.at[10]),
        pltpu.make_async_copy(out_ref.at[other_at, :], targets[6], sem.at[11]),
        pltpu.make_async_copy(out_ref, targets[7], sem.at[12]),
    ]
    for save in last:
        save.start()
    for save in saves + last:
        save.wait()


def attend(piece_start, piece_kind, tokens, gain, wq, wk, wv, table):
    rows, width = tokens.shape
    vmem = pl.BlockSpec(memory_space=pltpu.VMEM)
    smem = pl.BlockSpec(memory_space=pltpu.SMEM)

    def shape(*dims, dtype=BF16):
        return jax.ShapeDtypeStruct(dims, dtype)

    any_space = pl.BlockSpec(memory_space=pl.ANY)
    return pl.pallas_call(
        attend_kernel,
        out_shape=(
            shape(8, rows, dtype=F32),
            shape(rows, width),
            shape(4, rows, 128),
            shape(2, rows, 128),
            shape(2, rows, 128),
            shape(rows, 128, dtype=F32),
            shape(rows // 2, 256),
            shape(rows // 2, 256),
            shape(rows, 256),
        ),
        in_specs=[smem, smem, vmem] + [any_space] * 5,
        out_specs=(vmem,) + (any_space,) * 8,
        scratch_shapes=[
            pltpu.VMEM((rows, width), BF16),
            pltpu.VMEM((width, 256), BF16),
            pltpu.VMEM((width, 128), BF16),
            pltpu.VMEM((width, 128), BF16),
            pltpu.VMEM((rows, 128), F32),
            pltpu.VMEM((rows, width), BF16),
            pltpu.VMEM((4, rows, 128), BF16),
            pltpu.VMEM((2, rows, 128), BF16),
            pltpu.VMEM((2, rows, 128), BF16),
            pltpu.VMEM((rows, 128), F32),
            pltpu.VMEM((rows, 256), BF16),
            pltpu.VMEM((2, 128, rows), BF16),
            pltpu.SemaphoreType.DMA((13,)),
        ],
        compiler_params=pltpu.CompilerParams(vmem_limit_bytes=VMEM_BYTES),
        cost_estimate=pl.CostEstimate(
            flops=6 << 30, bytes_accessed=8 << 20, transcendentals=4 * rows * rows
        ),
        name="attend",
    )(piece_start, piece_kind, gain[None, :], tokens, wq, wk, wv, table)


def place_blocks(source, keep, send, ways, order, sems):
    me = lax.axis_index("dp")
    piece = source.shape[0] // ways
    half = ways // 2
    copies = []
    for slot in range(ways):
        dest = 0
        for place, bit in enumerate(order):
            own = (slot >> (len(order) - 1 - place)) & 1
            dest = dest + ((me // (1 << bit) + own) % 2) * (1 << bit)
        block = source.at[pl.ds(pl.multiple_of(dest * piece, piece), piece), :]
        target = keep.at[slot] if slot < half else send.at[slot - half]
        copies.append(pltpu.make_async_copy(block, target, sems.at[slot]))
    return copies


def attend_back_kernel(ways, order, start_ref, kind_ref, lse_ref, *refs):
    sources, refs = refs[:12], refs[12:]
    own_do, got_do, keep, send, dn_own, dn_other, gain_ref = refs[:7]
    held, refs = refs[7:15], refs[15:]
    qm_ref, k2_ref, v2_ref, o_ref, n1_ref, tok_ref, r1_ref, table_ref = held
    wo_ref, do, dom, do_t, n1_t, k2t, dk_acc, dv_acc, gqkv, wqkv, grads, dn, block_sem, sem = refs
    rows, width = tok_ref.shape
    scale = HEAD_SIZE ** (-0.5)
    core = lax.axis_index("tensor") % 2
    half = rows // 2
    own_at = pl.ds(pl.multiple_of(core * half, half), half)
    other_at = pl.ds(pl.multiple_of((1 - core) * half, half), half)
    loads = (
        pltpu.make_async_copy(own_do, do.at[own_at, :], sem.at[0]),
        pltpu.make_async_copy(got_do, do.at[other_at, :], sem.at[1]),
    )
    places = (wo_ref, k2_ref, n1_ref, qm_ref, v2_ref, table_ref, o_ref, tok_ref, r1_ref)
    places = places + (wqkv.at[:, :256], wqkv.at[:, 256:384], wqkv.at[:, 384:])
    more = [
        pltpu.make_async_copy(source, target, sem.at[2 + i])
        for i, (source, target) in enumerate(zip(sources, places))
    ]
    for load in list(loads) + more:
        load.start()
    dk_acc[...] = jnp.zeros_like(dk_acc)
    dv_acc[...] = jnp.zeros_like(dv_acc)
    for load in list(loads) + more[:3]:
        load.wait()

    def prepare(i, _):
        at = pl.ds(pl.multiple_of(i * SUB, SUB), SUB)
        block = do[at, :]
        dob = mm(block, wo_ref[...], ((1,), (1,)))
        for g in range(2):
            pair = dob[:, g * 128 : (g + 1) * 128]
            left = lanes_of(pair) < HEAD_SIZE
            dom[2 * g, at, :] = jnp.where(left, pair, 0.0).astype(BF16)
            dom[2 * g + 1, at, :] = jnp.where(left, 0.0, pair).astype(BF16)
            k2t[g, :, at] = k2_ref[g, at, :].T
        do_t[:, at] = block.T
        n1_t[:, at] = n1_ref[at, :].T
        return 0

    lax.fori_loop(0, rows // SUB, prepare, 0)
    for load in more[3:]:
        load.wait()
    for block in range(rows // QBLK):
        length = (block + 1) * QBLK

        def part(i, _):
            first_row = block * QBLK + i * SUB
            at = pl.ds(pl.multiple_of(first_row, SUB), SUB)
            visible = seen(start_ref, kind_ref, length, first_row)
            visible = jnp.concatenate([visible.astype(F32)] * 2, axis=1) > 0.0
            table = table_ref[at, :]
            for g in range(2):
                q = jnp.concatenate([qm_ref[2 * g, at, :], qm_ref[2 * g + 1, at, :]], axis=0)
                dob = jnp.concatenate([dom[2 * g, at, :], dom[2 * g + 1, at, :]], axis=0)
                lse = jnp.concatenate([lse_ref[2 * g : 2 * g + 1, at], lse_ref[2 * g + 1 : 2 * g + 2, at]], axis=1)
                scores = mm(k2_ref[g, :length, :], q, ((1,), (1,))) * scale
                probs = jnp.exp(jnp.where(visible, scores, negative) - lse)
                dp = mm(v2_ref[g, :length, :], dob, ((1,), (1,)))
                delta = jnp.sum(probs * dp, axis=0, keepdims=True)
                ds = (probs * (dp - delta)).astype(BF16)
                dk_acc[g, :length, :] += mm(ds, q, ((1,), (0,)))
                dv_acc[g, :length, :] += mm(probs.astype(BF16), dob, ((1,), (0,)))
                dq = mm(k2t[g, :, :length], ds, ((1,), (0,)))
                even = lax.broadcasted_iota(jnp.int32, (2 * HEAD_SIZE, SUB), 0) < HEAD_SIZE
                dq = jnp.where(even, dq[:, :SUB], dq[:, SUB:]).T * scale
                gqkv[at, g * 128 : (g + 1) * 128] = turn(dq, table, -1.0).astype(BF16)
            return 0

        lax.fori_loop(0, QBLK // SUB, part, 0)

    def close(i, _):
        at = pl.ds(pl.multiple_of(i * SUB, SUB), SUB)

        def folded(acc):
            first, second = acc[0, at, :], acc[1, at, :]
            left = lanes_of(first) < HEAD_SIZE
            first = first + pltpu.roll(first, HEAD_SIZE, 1)
            second = second + pltpu.roll(second, HEAD_SIZE, 1)
            return jnp.where(left, first, second)

        gqkv[at, 256:384] = turn(folded(dk_acc) * scale, table_ref[at, :], -1.0).astype(BF16)
        gqkv[at, 384:] = folded(dv_acc).astype(BF16)
        return 0

    lax.fori_loop(0, rows // SUB, close, 0)

    def weight_rows(i, _):
        at = pl.ds(pl.multiple_of(i * SUB, SUB), SUB)
        grads[at, :512] = mm(n1_t[at, :], gqkv[...], ((1,), (0,))).astype(BF16)
        grads[at, 512:] = mm(do_t[at, :], o_ref[...], ((1,), (0,))).astype(BF16)
        return 0

    lax.fori_loop(0, width // SUB, weight_rows, 0)
    copies = place_blocks(grads, keep, send, ways, order, block_sem)
    for copy in copies:
        copy.start()
    gain_ref[...] = jnp.zeros_like(gain_ref)

    def data_rows(i, _):
        at = pl.ds(pl.multiple_of(i * SUB, SUB), SUB)
        grad = mm(gqkv[at, :], wqkv[...], ((1,), (1,)))
        dn[at, :] = grad.astype(BF16)
        by = grad * (tok_ref[at, :].astype(F32) * r1_ref[at, :1])
        gain_ref[0:1, :] += jnp.sum(by, axis=0, keepdims=True)
        return 0

    lax.fori_loop(0, rows // SUB, data_rows, 0)
    saves = (
        pltpu.make_async_copy(dn.at[own_at, :], dn_own, sem.at[0]),
        pltpu.make_async_copy(dn.at[other_at, :], dn_other, sem.at[1]),
    )
    for copy in saves:
        copy.start()
    for copy in copies:
        copy.wait()
    for copy in saves:
        copy.wait()


def attend_back(ways, order, piece_start, piece_kind, saved, tokens, weights, table, own_do, got_do):
    lse, n1, qm, k2, v2, r1, _, _, out = saved
    wq, wk, wv, wo = weights
    rows, width = tokens.shape
    vmem = pl.BlockSpec(memory_space=pltpu.VMEM)
    smem = pl.BlockSpec(memory_space=pltpu.SMEM)
    any_space = pl.BlockSpec(memory_space=pl.ANY)
    block = jax.ShapeDtypeStruct((ways // 2, width // ways, 768), BF16)
    half = jax.ShapeDtypeStruct((rows // 2, width), BF16)
    return pl.pallas_call(
        functools.partial(attend_back_kernel, ways, order),
        out_shape=(block, block, half, half, jax.ShapeDtypeStruct((8, width), F32)),
        in_specs=[smem, smem, vmem] + [any_space] * 14,
        out_specs=(any_space,) * 4 + (vmem,),
        scratch_shapes=[
            pltpu.VMEM((4, rows, 128), BF16),
            pltpu.VMEM((2, rows, 128), BF16),
            pltpu.VMEM((2, rows, 128), BF16),
            pltpu.VMEM((rows, 256), BF16),
            pltpu.VMEM((rows, width), BF16),
            pltpu.VMEM((rows, width), BF16),
            pltpu.VMEM((rows, 128), F32),
            pltpu.VMEM((rows, 128), F32),
            pltpu.VMEM((256, width), BF16),
            pltpu.VMEM((rows, width), BF16),
            pltpu.VMEM((4, rows, 128), BF16),
            pltpu.VMEM((width, rows), BF16),
            pltpu.VMEM((width, rows), BF16),
            pltpu.VMEM((2, 128, rows), BF16),
            pltpu.VMEM((2, rows, 128), F32),
            pltpu.VMEM((2, rows, 128), F32),
            pltpu.VMEM((rows, 512), BF16),
            pltpu.VMEM((width, 512), BF16),
            pltpu.VMEM((width, 768), BF16),
            pltpu.VMEM((rows, width), BF16),
            pltpu.SemaphoreType.DMA((ways,)),
            pltpu.SemaphoreType.DMA((14,)),
        ],
        compiler_params=pltpu.CompilerParams(vmem_limit_bytes=VMEM_BYTES),
        cost_estimate=pl.CostEstimate(
            flops=12 << 30, bytes_accessed=16 << 20, transcendentals=4 * rows * rows
        ),
        name="attend_back",
    )(piece_start, piece_kind, lse, wo, k2, n1, qm, v2, table, out, tokens, r1, wq, wk, wv, own_do, got_do)


def make_body(ways):
    def body(
        tokens,
        w_query,
        key_weight,
        value_weight,
        w_output,
        gain_attn,
        gain_ffn,
        router,
        w_gate,
        w_up,
        w_down,
        piece_start,
        piece_kind,
        choices,
        place_order,
        cotangent,
    ):
        rows = tokens.shape[0]
        half = rows // 2
        width = tokens.shape[1]
        core = lax.axis_index("tensor") % 2

        def my_half(array):
            return lax.dynamic_slice_in_dim(array, core * half, half, 0)

        from_x = lax.ppermute(w_output, "tensor", X_PAIRS)
        from_core = lax.ppermute(w_output, "tensor", CORE_PAIRS)
        from_both = lax.ppermute(from_x, "tensor", CORE_PAIRS)
        resid_in = tokens.astype(F32)
        table = jnp.asarray(rope_packed(rows))
        saved = attend(
            piece_start, piece_kind, tokens, gain_attn, w_query, key_weight, value_weight, table
        )
        mine, other = saved[6], saved[7]
        far_mine = lax.ppermute(mine, "tensor", X_PAIRS)
        got = lax.ppermute(other, "tensor", CORE_PAIRS)
        far_got = lax.ppermute(got, "tensor", X_PAIRS)
        near_heads = jnp.concatenate([mine, got], axis=1)
        near_output = jnp.concatenate([w_output, from_core], axis=0)
        near = my_half(resid_in) + mm(near_heads, near_output, ((1,), (0,)))
        far_output = jnp.concatenate([from_x, from_both], axis=0)
        far_heads = jnp.concatenate([far_mine, far_got], axis=1)
        mid = near + mm(far_heads, far_output, ((1,), (0,)))
        inv_two = lax.rsqrt(jnp.mean(mid * mid, axis=1, keepdims=True) + epsilon)
        normed_half = (mid * inv_two * gain_ffn).astype(BF16)
        normed_far = lax.ppermute(normed_half, "tensor", CORE_PAIRS)

        expert_ids = jnp.arange(E, dtype=jnp.int32)
        picked = jnp.any(choices[:, :, None] == expert_ids[None, None, :], axis=1)
        ranks = place_order[0]
        earlier = (ranks[None, :] < ranks[:, None]).astype(BF16)
        slot = mm(earlier, picked.astype(BF16), ((1,), (0,)))
        kept = (picked & (slot < CAP)).astype(F32)
        picked_half = my_half(picked.astype(F32))
        kept_half = my_half(kept)
        logits = mm(normed_half, router, ((1,), (0,)))
        logits = jnp.where(picked_half > 0, logits, negative)
        gates_half = jax.nn.softmax(logits, axis=1)
        gates_half = jnp.where(picked_half > 0, gates_half, 0.0)
        slot_gate = gates_half * kept_half
        slot_gate_far = lax.ppermute(slot_gate, "tensor", CORE_PAIRS)

        piece = width // ways
        ff = w_gate.shape[2]
        plain = bits_of(ways)
        turned = plain[1:] + plain[:1]
        shared = (slot_gate, slot_gate_far, normed_half, normed_far, cotangent, w_gate, w_up, w_down)
        orders = (plain, turned, plain, plain)
        carry = None
        dg_parts, keeps, gots = [], [], []
        for quad in range(E // QUAD):
            result = run_experts(quad, orders[quad], ways, *shared, carry)
            if quad == E // QUAD - 1:
                dg_part, *halves, keep, send = result
            else:
                dg_part, norm_part, moe_part, keep, send = result[:5]
                carry = (tuple(result[5:]) if quad == 0 else carry[:2]) + (norm_part, moe_part)
            dg_parts.append(dg_part[:, quad * QUAD : (quad + 1) * QUAD])
            keep, got = halve(keep, send, ways, orders[quad])
            keeps.append(keep)
            gots.append(got)
        sent_gate, sent_up, sent_down = unpack(keeps, gots, ff)
        grad_gate_part = jnp.concatenate(dg_parts, axis=1) * kept

        norm_near, norm_far = reduce_pair(halves[0], halves[1])
        norm_half = norm_near.astype(F32) + norm_far.astype(F32)
        dg_other = lax.dynamic_slice_in_dim(grad_gate_part, (1 - core) * half, half, 0).astype(BF16)
        dg_near, dg_far = reduce_pair(my_half(grad_gate_part), dg_other)
        dg_half = dg_near.astype(F32) + dg_far.astype(F32)
        moe_near, moe_far = reduce_pair(halves[2], halves[3])
        dz = gates_half * (dg_half - jnp.sum(gates_half * dg_half, axis=1, keepdims=True))
        dlg = dz.astype(BF16)
        grad_norm = norm_half + mm(dlg, router, ((1,), (1,)))
        grad_router = mm(dlg, normed_half, ((0,), (0,)))
        grad_gain_ffn = jnp.sum(grad_norm * mid * inv_two, axis=0)
        scaled = gain_ffn * grad_norm
        grad_mid = (
            my_half(cotangent).astype(F32)
            + inv_two * scaled
            - mid * inv_two**3 * jnp.mean(scaled * mid, axis=1, keepdims=True)
        )
        own_do = grad_mid.astype(BF16)
        got_do = lax.ppermute(own_do, "tensor", CORE_PAIRS)
        keep, send, dn_own, dn_other, gain_rows = attend_back(
            ways,
            plain,
            piece_start,
            piece_kind,
            saved,
            tokens,
            (w_query, key_weight, value_weight, w_output),
            table,
            own_do,
            got_do,
        )
        grad_gain_attn = gain_rows[0]
        moe_far, dn_own = lax.optimization_barrier((moe_far, dn_own))
        output = (mid + (moe_near.astype(F32) + moe_far.astype(F32))).astype(BF16)
        output = share_half(output, core)
        keep, got = halve(keep, send, ways, plain)
        sent_attn = keep[0].astype(F32) + got[0].astype(F32)
        nq, nk = w_query.shape[1], key_weight.shape[1]
        last_near, last_far = reduce_pair(dn_own, dn_other)
        norm_one_half = last_near.astype(F32) + last_far.astype(F32)
        x_half = my_half(resid_in)
        inv_half = lax.rsqrt(jnp.mean(x_half * x_half, axis=1, keepdims=True) + epsilon)
        scaled_one = gain_attn * norm_one_half
        input_half = (
            grad_mid
            + inv_half * scaled_one
            - x_half * inv_half**3 * jnp.mean(scaled_one * x_half, axis=1, keepdims=True)
        ).astype(BF16)
        input_grad = share_half(input_half, core)
        first_chip = (lax.axis_index("tensor") < 2).astype(F32)
        row_sums = jnp.concatenate([grad_gain_ffn[None], grad_router], axis=0) * first_chip
        small = jnp.concatenate([grad_gain_attn[None], row_sums], axis=0)
        small = small + lax.ppermute(small, "tensor", CORE_PAIRS)
        small = small + lax.ppermute(small, "tensor", X_PAIRS)
        count = small.shape[0]
        small = small.reshape(count, ways, piece).transpose(1, 0, 2)
        (small,) = scatter_sums((small,), ways, plain)
        return (
            output,
            input_grad,
            sent_attn[:, :nq],
            sent_attn[:, nq : nq + nk],
            sent_attn[:, nq + nk : nq + 2 * nk],
            sent_attn[:, nq + 2 * nk :].T,
            small[0],
            small[1],
            small[2:].T,
            sent_gate,
            sent_up,
            sent_down,
        )

    return body


def solution(mesh):
    body = make_body(mesh.shape["dp"])

    return jax.shard_map(
        body,
        mesh=mesh,
        in_specs=(
            P("dp", None),
            P(None, "tensor"),
            P(None, "tensor"),
            P(None, "tensor"),
            P("tensor", None),
            P(),
            P(),
            P(),
            P(None, None, "tensor"),
            P(None, None, "tensor"),
            P(None, "tensor", None),
            P("dp", None),
            P("dp", None),
            P("dp", None),
            P("dp", None),
            P("dp", None),
        ),
        out_specs=(
            P("dp", None),
            P("dp", None),
            P("dp", "tensor"),
            P("dp", "tensor"),
            P("dp", "tensor"),
            P("tensor", "dp"),
            P("dp"),
            P("dp"),
            P("dp", None),
            P(None, "dp", "tensor"),
            P(None, "dp", "tensor"),
            P(None, "tensor", "dp"),
        ),
        check_vma=False,
    )
```
